128 devices in a mesh: dp: 4 (over z_hi, core), ep: 32 (over x, z_lo, y).
Axes of the slice: x: 4, y: 4, z: 4 (z_hi: 2, z_lo: 2; z = z_hi * 2 + z_lo), core: 2. Of those that a mesh axis runs over, the one named last changes fastest.
Arguments:
- tokens: bfloat16 [16384, 2048], P(('dp', 'ep')), parts along dimension 0, may hold values from -6 to 6
- expert_ids: int32 [16384, 8], P(('dp', 'ep')), parts along dimension 0, may hold values from 0 to 63, all different within a row; in each aligned block of 32 rows (0 to 31, 32 to 63, ...) at most 8 rows name the same one
- gate_nums: int32 [16384, 8], P(('dp', 'ep')), parts along dimension 0, may hold values from 64 to 1023
- w_gate: bfloat16 [64, 2048, 768], P('ep'), may hold values from -0.125 to 0.125
- w_up: bfloat16 [64, 2048, 768], P('ep'), may hold values from -0.125 to 0.125
- w_down: bfloat16 [64, 768, 2048], P('ep'), may hold values from -0.21875 to 0.21875
Outputs:
- mixed: bfloat16 [16384, 2048], P(('dp', 'ep')), parts along dimension 0
The draws below stay inside these ranges and needn't reach their ends.
There are 4 independent parts, one for each index of `dp`. The reference program is written for one: setup_inputs(seed, part) draws one part's arguments, and reference() takes and returns one part's arrays. A program takes and returns all parts, laid end to end along the dimension named above; an argument that names none is the same for every part. Nothing has to cross between parts.
Inputs may be any that keep to these rules, and one draw needn't show every extreme that they name: `expert_ids`: each row names 8 different experts. In every aligned block of 32 rows no expert is named by more than 8 rows, a bound that some block reaches.
All inputs are finite; a program needn't handle non-finite values.
Results may differ from the reference program's by a relative error of at most 0.008.
Values may be sent and summed in bfloat16 or wider, within the bound.
A program may use at most 128 MiB of HBM per device.

```python
import math
import jax
import jax.numpy as jnp
import numpy as np
from jax import lax

D = 2048
FF = 768
TOP = 8
EXPERTS = 64
TOKENS = 4096
BLK = 32
CAP = 8


def touch_ends(array, own_key, least, high):
    extent = array.shape
    place = [jax.random.randint(jax.random.fold_in(own_key, axis), (), 0, extent[axis]) for axis in range(len(extent))]
    array = array.at[tuple(place)].set(least)
    longest = extent.index(max(extent))
    place[longest] = (place[longest] + 1) % extent[longest]
    return array.at[tuple(place)].set(high)


def steps_of(own_key, shape, split, low, largest):
    def one(axis_at, parts):
        steps = jax.random.uniform(jax.random.fold_in(jax.random.fold_in(own_key, 6), axis_at), (parts,), jnp.float32, low / len(split), largest / len(split))
        return jnp.repeat(jnp.exp(steps), shape[axis_at] // parts).reshape((-1,) + (1,) * (len(shape) - axis_at - 1))

    level = one(*split[0])
    for cut in split[1:]:
        level = level * one(*cut)
    return level


def deal_out(own_key, own, number, rows, count, top, most, lean):
    order = jax.random.permutation(own_key, count)
    heavy_load, ordinary = shares(count, rows * top, most, lean, True), shares(count, rows * top, most, lean, False)
    places = jnp.arange(count)

    def named(tallies, rotation):
        used = int((tallies > 0).sum())
        fixed = max(1, used // 4)
        moved = fixed + (places - fixed + rotation * (used - fixed)) % max(1, count - fixed)
        return jnp.zeros((count,), jnp.int32).at[order[jnp.where(places < fixed, places, moved)]].set(jnp.asarray(tallies, jnp.int32))

    tallies = jnp.where(number % 4 == 0, named(heavy_load, number // 4), named(ordinary, number - number // 4 - 1))
    mixed = jax.random.permutation(jax.random.fold_in(own, 3), count)
    source_of, sink = mixed[0:count // 2 * 2:2], mixed[1:count // 2 * 2:2]
    margin = jnp.minimum(tallies[source_of] - 1, most - tallies[sink]) // 2
    margin = jnp.where((source_of == order[0]) | (sink == order[0]) | (tallies[sink] == 0), 0, jnp.maximum(margin, 0))
    moved = jax.random.randint(jax.random.fold_in(own, 4), (count // 2,), 0, 1 << 20) % (margin + 1)
    tallies = tallies.at[source_of].add(-moved).at[sink].add(moved)
    members = jnp.searchsorted(jnp.cumsum(tallies), jnp.arange(rows * top), side="right").astype(jnp.int32)
    table = members.reshape(top, rows).T
    table = table[jax.random.permutation(jax.random.fold_in(own, 1), rows)]
    rotation = jax.random.randint(jax.random.fold_in(own, 2), (rows, 1), 0, top)
    return jnp.take_along_axis(table, (jnp.arange(top)[None, :] + rotation) % top, axis=1)


def shares(amount, total, bound, lean, full):
    loads = [(1 << 20) // math.isqrt(rank ** lean) + 1 for rank in range(1, amount + 1)]
    largest = bound if full else min(bound, max(-(-total // amount), total * loads[0] // sum(loads)))
    least = 1 if total - largest >= amount - 1 else 0
    holding, surplus = [largest] + [least] * (amount - 1), total - largest - least * (amount - 1)
    while surplus > 0:
        movable = [i for i in range(1, amount) if holding[i] < largest] or [i for i in range(1, amount) if holding[i] < bound]
        mass, budget = sum([loads[i] for i in movable]), surplus
        for i in movable:
            addition = min(bound - holding[i], max(1, budget * loads[i] // mass), surplus)
            holding[i] = holding[i] + addition
            surplus = surplus - addition
    return np.array(holding)


def noise(rng, extent, deviation, limit, shards=(), held_as=jnp.bfloat16):
    entries = deviation * jax.random.normal(rng, extent, jnp.float32)
    if shards:
        entries = entries * steps_of(rng, extent, shards, -0.22, 0.18)
    return jnp.clip(entries, -limit, limit).astype(held_as)


def setup_inputs(seed: int = 0, part: int = 0) -> dict:
    keys = jax.random.split(jax.random.key(seed), 7)
    part_keys = jax.random.split(jax.random.fold_in(keys[6], part), 7)
    tokens = noise(part_keys[0], (TOKENS, D), 1.0, 6.0, ((0, 32),))
    expert_ids_keys = jax.random.split(jax.random.fold_in(part_keys[1], 1), TOKENS // BLK)
    expert_ids_turns = jax.random.permutation(jax.random.fold_in(part_keys[1], 3), TOKENS // BLK)
    expert_ids = jax.vmap(lambda own, number: deal_out(jax.random.fold_in(part_keys[1], 2), own, number, BLK, EXPERTS, TOP, CAP, 2))(expert_ids_keys, expert_ids_turns).reshape((TOKENS, TOP))
    gate_nums = touch_ends(jax.random.randint(part_keys[2], (TOKENS, TOP), 64, 1024), jax.random.fold_in(part_keys[2], 1), 64, 1023).astype(jnp.int32)
    w_gate = noise(keys[3], (EXPERTS, D, FF), D ** -0.5, 0.125, ((0, 32),))
    w_up = noise(keys[4], (EXPERTS, D, FF), D ** -0.5, 0.125, ((0, 32),))
    w_down = noise(keys[5], (EXPERTS, FF, D), FF ** -0.5, 0.21875, ((0, 32),))
    return {"tokens": tokens, "expert_ids": expert_ids, "gate_nums": gate_nums, "w_gate": w_gate, "w_up": w_up, "w_down": w_down}


denominator = 1024.0


def reference(tokens, expert_ids, gate_nums, w_gate, w_up, w_down):
    total = tokens.shape[0]
    most = CAP * (total // BLK)
    gates = gate_nums.astype(jnp.float32) / denominator

    def step(accum, expert):
        hit = expert_ids == expert
        weight = jnp.sum(jnp.where(hit, gates, jnp.zeros_like(gates)), axis=1)
        member = jnp.any(hit, axis=1)
        index = jnp.nonzero(member, size=most, fill_value=0)[0].astype(jnp.int32)
        valid = jnp.arange(most, dtype=jnp.int32) < jnp.sum(member.astype(jnp.int32))
        picked = tokens[index]
        gate = jnp.dot(picked, w_gate[expert], preferred_element_type=jnp.float32)
        up = jnp.dot(picked, w_up[expert], preferred_element_type=jnp.float32)
        hidden = (jax.nn.silu(gate) * up).astype(jnp.bfloat16)
        result = jnp.dot(hidden, w_down[expert], preferred_element_type=jnp.float32).astype(jnp.bfloat16)
        scale = jnp.where(valid, weight[index], jnp.zeros_like(weight[index]))
        accum = accum.at[index].add(scale[:, None] * result.astype(jnp.float32))
        return accum, None

    start = jnp.zeros((total, tokens.shape[1]), jnp.float32)
    accum, _ = lax.scan(step, start, jnp.arange(EXPERTS, dtype=jnp.int32))
    return accum.astype(jnp.bfloat16)
```

```python
import jax
import jax.numpy as jnp
from jax import lax
from jax.experimental import pallas as pl
from jax.experimental.pallas import tpu as pltpu
from jax.sharding import PartitionSpec as P

MESH = pl.DeviceIdType.MESH
BF = jnp.bfloat16
F32 = jnp.float32
D = 2048
FF = 768
TOK = 128
HALF = 64
CAP = 32
ORDER = (0, 3, 1, 2)
BACK = (2, 1, 3, 0)


def neighbours():
    dp, ep = lax.axis_index("dp"), lax.axis_index("ep")
    z_hi, core = dp // 2, dp % 2
    x, z_lo, y = ep // 8, (ep // 4) % 2, ep % 4
    z = z_hi * 2 + z_lo
    a = (1 - core) * x + core * y
    b = (1 - core) * y + core * x

    def device(a, b, z):
        px = (1 - core) * a + core * b
        py = (1 - core) * b + core * a
        return ((z // 2) * 2 + core, (px * 2 + z % 2) * 4 + py)

    up = z + 1 - 2 * (z % 2)
    down = (z + 3 + 2 * (z % 2)) % 4
    zp = (1 - core) * up + core * down
    where = {
        "a+": device((a + 1) % 4, b, z),
        "a-": device((a + 3) % 4, b, z),
        "b+": device(a, (b + 1) % 4, z),
        "b-": device(a, (b + 3) % 4, z),
        "z": device(a, b, zp),
    }
    return where, ep, where["z"][1]


def kernel(
    tokens, meta, wg_in, wu_in, wd_in, out,
    wg, wu, wd, T, M, X, ZS, YR, PS, G, H, FAR, ADJ, FFR, FA, TRI,
    send, recv, local, wsem,
):
    where, ep, pep = neighbours()
    counter = [0]

    def remote(src, dst, to):
        index = counter[0]
        counter[0] += 1
        return pltpu.make_async_remote_copy(
            src_ref=src, dst_ref=dst, send_sem=send.at[index], recv_sem=recv.at[index],
            device_id=where[to], device_id_type=MESH,
        )

    loads = [
        pltpu.make_async_copy(src.at[e], dst.at[e], wsem.at[k, e])
        for e in range(2)
        for k, (src, dst) in enumerate(((wg_in, wg), (wu_in, wu), (wd_in, wd)))
    ]
    own = pltpu.make_async_copy(tokens, T.at[0, 0], local.at[0])
    own_meta = pltpu.make_async_copy(meta, M.at[0, 0, 0], local.at[1])
    own.start()
    own_meta.start()
    for load in loads:
        load.start()

    mz = remote(M.at[0, 0, 0], M.at[0, 0, 1], "z")
    mf = [
        remote(M.at[0, 0], M.at[0, 3], "a+"),
        remote(M.at[0, 0], M.at[0, 1], "a-"),
        remote(M.at[0, 3], M.at[0, 2], "a+"),
    ]
    ms = [
        remote(M.at[0], M.at[3], "b+"),
        remote(M.at[0], M.at[1], "b-"),
        remote(M.at[3], M.at[2], "b+"),
    ]
    f = {
        (3, 0): remote(T.at[0, 0, 0], T.at[0, 3, 0], "a+"),
        (3, 1): remote(T.at[0, 0, 1], T.at[0, 3, 1], "a+"),
        (2, 0): remote(T.at[0, 3, 0], T.at[0, 2, 0], "a+"),
        (1, 1): remote(T.at[0, 0, 1], T.at[0, 1, 1], "a-"),
        (1, 0): remote(T.at[0, 0, 0], T.at[0, 1, 0], "a-"),
        (2, 1): remote(T.at[0, 1, 1], T.at[0, 2, 1], "a-"),
    }
    s = {}
    for i in range(4):
        s[2, i, 0] = remote(T.at[0, i, 0], T.at[2, i, 0], "b+")
        s[2, i, 1] = remote(T.at[0, i, 1], T.at[2, i, 1], "b-")
        s[1, i, 0] = remote(T.at[2, i, 0], T.at[1, i, 0], "b+")
        s[1, i, 1] = remote(T.at[2, i, 1], T.at[1, i, 1], "b-")
        s[3, i, 1] = remote(T.at[0, i, 1], T.at[3, i, 1], "b+")
        s[3, i, 0] = remote(T.at[0, i, 0], T.at[3, i, 0], "b-")
    zs = {(c, i): remote(ZS.at[c, i], X.at[c, 1, i], "z") for c in range(4) for i in range(4)}
    zr = {(c, i): remote(X.at[c, 1, i], YR.at[c, i], "z") for c in range(4) for i in range(4)}
    far = {}
    adj = {}
    for i in range(4):
        far[i, 0] = remote(T.at[1, i, 0], FAR.at[i, 0], "b+")
        far[i, 1] = remote(T.at[1, i, 1], FAR.at[i, 1], "b-")
        adj[2, i, 0] = remote(T.at[2, i, 0], ADJ.at[1, i, 0], "b-")
        adj[2, i, 1] = remote(T.at[2, i, 1], ADJ.at[0, i, 1], "b+")
        adj[3, i, 0] = remote(T.at[3, i, 0], ADJ.at[0, i, 0], "b+")
        adj[3, i, 1] = remote(T.at[3, i, 1], ADJ.at[1, i, 1], "b-")
    ff = {
        0: remote(T.at[0, 2, 0], FFR.at[0], "a+"),
        1: remote(T.at[0, 2, 1], FFR.at[1], "a-"),
    }
    fa = {
        (1, 0): remote(T.at[0, 1, 0], FA.at[0, 0], "a+"),
        (1, 1): remote(T.at[0, 1, 1], FA.at[0, 1], "a+"),
        (3, 0): remote(T.at[0, 3, 0], FA.at[1, 0], "a-"),
        (3, 1): remote(T.at[0, 3, 1], FA.at[1, 1], "a-"),
    }

    barrier = pltpu.get_barrier_semaphore()
    for name in ("a+", "a-", "b+", "b-", "z"):
        pl.semaphore_signal(barrier, inc=1, device_id=where[name], device_id_type=MESH)

    lane = lax.broadcasted_iota(jnp.int32, (TOK, TOK), 1)
    row = lax.broadcasted_iota(jnp.int32, (TOK, TOK), 0)
    TRI[...] = jnp.where((row < lane) & ((row & 96) == (lane & 96)), 1.0, 0.0).astype(BF)
    own_meta.wait()
    own.wait()
    pl.semaphore_wait(barrier, 5)

    mz.start()
    f[3, 0].start()
    f[1, 1].start()
    s[2, 0, 0].start()
    s[2, 0, 1].start()
    f[3, 1].start()
    f[1, 0].start()

    sub8 = lax.broadcasted_iota(jnp.int32, (8, TOK), 0)
    lane8 = lax.broadcasted_iota(jnp.int32, (8, TOK), 1)
    sub32 = lax.broadcasted_iota(jnp.int32, (CAP, TOK), 0).astype(F32)
    expert = jnp.where(
        sub8 < 2, 2 * ep + sub8, jnp.where(sub8 < 4, 2 * pep + sub8 - 2, 2 * ep + sub8 - 4)
    )
    start_slot = ((lane8 & 96) >> 2).astype(F32)

    def pick(c, i, plane):
        if c == 0:
            return M[0, i, plane]
        if c == 1:
            return M[2, i, plane]
        low = lax.broadcasted_iota(jnp.int32, (16, TOK), 1) < HALF
        first, second = (3, 1) if c == 2 else (1, 3)
        return jnp.where(low, M[first, i, plane], M[second, i, plane])

    def pack(c, i):
        mine, theirs = pick(c, i, 0), pick(c, i, 1)
        member = jnp.zeros((8, TOK), F32)
        weight = jnp.zeros((8, TOK), jnp.int32)
        for k in range(8):
            ids = jnp.where(sub8 < 4, mine[k : k + 1], theirs[k : k + 1])
            nums = jnp.where(sub8 < 4, mine[8 + k : 9 + k], theirs[8 + k : 9 + k])
            hit = ids == expert
            member = member + jnp.where(hit, 1.0, 0.0)
            weight = weight + jnp.where(hit, nums, 0)
        before = jnp.dot(member.astype(BF), TRI[...], preferred_element_type=F32)
        code = jnp.where(member > 0.5, start_slot + before, -1.0)
        gate = weight.astype(F32) * (1.0 / 1024.0)
        hits = [sub32 == code[r : r + 1] for r in range(6)]
        places = jnp.concatenate([jnp.where(hits[r], 1.0, 0.0) for r in range(4)], axis=0).astype(BF)
        PS[c, i] = places
        for plane in range(2):
            for e in range(2):
                r = 4 * plane + e
                column = jnp.sum(jnp.where(hits[r], gate[r : r + 1], 0.0), axis=1, keepdims=True)
                G[c, e, plane, i] = jnp.broadcast_to(column, (CAP, TOK))
        for n in range(4):
            cols = slice(512 * n, 512 * n + 512)
            rows = T[c, i, :, :, cols].reshape(TOK, 512)
            packed = jnp.dot(places, rows, preferred_element_type=F32).astype(BF)
            X[c, 0, i, :, :, cols] = packed[:HALF].reshape(2, CAP, 512)
            ZS[c, i, :, :, cols] = packed[HALF:].reshape(2, CAP, 512)
        zs[c, i].start()

    def experts(c):
        for e in range(2):

            def gate_up(n, carry):
                cols = pl.ds(pl.multiple_of(n * 256, 256), 256)
                x = X[c, :, :, e].reshape(256, D)
                g = jnp.dot(x, wg[e, :, cols], preferred_element_type=F32)
                u = jnp.dot(x, wu[e, :, cols], preferred_element_type=F32)
                scale = G[c, e].reshape(256, TOK)[:, :1]
                H[:, cols] = (g / (1.0 + jnp.exp(-g)) * u * scale).astype(BF)
                return carry

            def down(n, carry):
                cols = pl.ds(pl.multiple_of(n * 512, 512), 512)
                y = jnp.dot(H[...], wd[e, :, cols], preferred_element_type=F32)
                X[c, :, :, e, :, cols] = y.astype(BF).reshape(2, 4, CAP, 512)
                return carry

            lax.fori_loop(0, 3, gate_up, 0)
            lax.fori_loop(0, 4, down, 0)

    def combine(c, i, extra, target=None):
        for n in range(4):
            cols = slice(512 * n, 512 * n + 512)
            y = jnp.concatenate(
                [X[c, 0, i, :, :, cols].reshape(HALF, 512), YR[c, i, :, :, cols].reshape(HALF, 512)], axis=0
            )
            total = lax.dot_general(PS[c, i], y, (((0,), (0,)), ((), ())), preferred_element_type=F32)
            for part in extra:
                total = total + part[:, :, cols].reshape(TOK, 512).astype(F32)
            if target is None:
                T[c, i, :, :, cols] = total.astype(BF).reshape(2, HALF, 512)
            else:
                target[:, cols] = total.astype(BF)

    mz.wait_recv()
    mf[0].start()
    mf[1].start()
    pack(0, 0)
    f[3, 0].wait_recv()
    f[2, 0].start()
    s[2, 3, 0].start()
    f[1, 1].wait_recv()
    f[2, 1].start()
    s[2, 1, 1].start()
    mf[0].wait_recv()
    mf[2].start()
    mf[1].wait_recv()
    f[1, 0].wait_recv()
    s[2, 1, 0].start()
    f[3, 1].wait_recv()
    s[2, 3, 1].start()
    mf[2].wait_recv()
    ms[0].start()
    ms[1].start()
    pack(0, 3)
    pack(0, 1)
    f[2, 0].wait_recv()
    s[2, 2, 0].start()
    f[2, 1].wait_recv()
    s[2, 2, 1].start()
    ms[0].wait_recv()
    ms[2].start()
    ms[1].wait_recv()
    pack(0, 2)
    for i in ORDER:
        s[2, i, 0].wait_recv()
        s[1, i, 0].start()
        s[2, i, 1].wait_recv()
        s[1, i, 1].start()
        pack(2, i)
    for i in ORDER:
        s[3, i, 1].start()
        s[3, i, 0].start()
    ms[2].wait_recv()

    for load in loads:
        load.wait()
    for i in ORDER:
        zs[0, i].wait_recv()
    experts(0)
    for i in ORDER:
        s[1, i, 0].wait_recv()
        s[1, i, 1].wait_recv()
        pack(1, i)
    for i in ORDER:
        zs[2, i].wait_recv()
    experts(2)
    for i in BACK:
        zr[2, i].start()
    for i in ORDER:
        s[3, i, 0].wait_recv()
        s[3, i, 1].wait_recv()
        pack(3, i)
    for i in ORDER:
        zs[1, i].wait_recv()
    experts(1)
    for i in BACK:
        zr[1, i].start()
    for copy in list(f.values()) + list(s.values()):
        copy.wait_send()
    for i in BACK:
        zr[2, i].wait_recv()
        combine(2, i, [])
        adj[2, i, 0].start()
        adj[2, i, 1].start()
    for i in ORDER:
        zs[3, i].wait_recv()
    experts(3)
    for i in BACK:
        zr[3, i].start()
    for i in BACK:
        zr[0, i].start()
    for i in BACK:
        zr[1, i].wait_recv()
        combine(1, i, [])
        far[i, 0].start()
        far[i, 1].start()
    for i in BACK:
        zr[3, i].wait_recv()
        far[i, 0].wait_recv()
        far[i, 1].wait_recv()
        combine(3, i, [FAR.at[i]])
        adj[3, i, 0].start()
        adj[3, i, 1].start()
    for i in BACK:
        zr[0, i].wait_recv()
        for c in (2, 3):
            adj[c, i, 0].wait_recv()
            adj[c, i, 1].wait_recv()
        if i:
            combine(0, i, [ADJ.at[0, i], ADJ.at[1, i]])
        if i == 2:
            ff[0].start()
            ff[1].start()
        if i == 1:
            fa[1, 1].start()
            ff[0].wait_recv()
            T[0, 1, 0] = (T[0, 1, 0].astype(F32) + FFR[0].astype(F32)).astype(BF)
            fa[1, 0].start()
        if i == 3:
            fa[3, 0].start()
            ff[1].wait_recv()
            T[0, 3, 1] = (T[0, 3, 1].astype(F32) + FFR[1].astype(F32)).astype(BF)
            fa[3, 1].start()
    for copy in fa.values():
        copy.wait_recv()
    combine(0, 0, [ADJ.at[0, 0], ADJ.at[1, 0], FA.at[0], FA.at[1]], out)

    for copy in [mz, *mf, *ms, *zs.values(), *zr.values(), *far.values(), *adj.values(), *ff.values(), *fa.values()]:
        copy.wait_send()


COPIES = 7 + 6 + 24 + 16 + 16 + 8 + 16 + 2 + 4


def shards(tokens, expert_ids, gate_nums, w_gate, w_up, w_down):
    meta = jnp.concatenate([expert_ids.T, gate_nums.T], axis=0)
    anywhere = pl.BlockSpec(memory_space=pl.ANY)
    return pl.pallas_call(
        kernel,
        name="routed_experts",
        out_shape=jax.ShapeDtypeStruct((TOK, D), BF),
        in_specs=[anywhere] * 5,
        out_specs=pl.BlockSpec(memory_space=pltpu.VMEM),
        scratch_shapes=[
            pltpu.VMEM((2, D, FF), BF),
            pltpu.VMEM((2, D, FF), BF),
            pltpu.VMEM((2, FF, D), BF),
            pltpu.VMEM((4, 4, 2, HALF, D), BF),
            pltpu.VMEM((4, 4, 2, 16, TOK), jnp.int32),
            pltpu.VMEM((4, 2, 4, 2, CAP, D), BF),
            pltpu.VMEM((4, 4, 2, CAP, D), BF),
            pltpu.VMEM((4, 4, 2, CAP, D), BF),
            pltpu.VMEM((4, 4, TOK, TOK), BF),
            pltpu.VMEM((4, 2, 2, 4, CAP, TOK), F32),
            pltpu.VMEM((256, FF), BF),
            pltpu.VMEM((4, 2, HALF, D), BF),
            pltpu.VMEM((2, 4, 2, HALF, D), BF),
            pltpu.VMEM((2, HALF, D), BF),
            pltpu.VMEM((2, 2, HALF, D), BF),
            pltpu.VMEM((TOK, TOK), BF),
            pltpu.SemaphoreType.DMA((COPIES,)),
            pltpu.SemaphoreType.DMA((COPIES,)),
            pltpu.SemaphoreType.DMA((2,)),
            pltpu.SemaphoreType.DMA((3, 2)),
        ],
        compiler_params=pltpu.CompilerParams(
            collective_id=0, has_side_effects=True, vmem_limit_bytes=67043328
        ),
    )(tokens.reshape(2, HALF, D), meta, w_gate, w_up, w_down)


def solution(mesh):
    placed = (
        P(("dp", "ep"), None),
        P(("dp", "ep"), None),
        P(("dp", "ep"), None),
        P("ep", None, None),
        P("ep", None, None),
        P("ep", None, None),
    )
    return jax.shard_map(
        shards, mesh=mesh, in_specs=placed, out_specs=P(("dp", "ep"), None), check_vma=False
    )
```

```python
import jax
import jax.numpy as jnp
from jax import lax
from jax.experimental import pallas as pl
from jax.experimental.pallas import tpu as pltpu
from jax.sharding import PartitionSpec as P

MESH = pl.DeviceIdType.MESH
BF = jnp.bfloat16
F32 = jnp.float32
D = 2048
FF = 768
TOK = 128
HALF = 64
CAP = 32
ORDER = (0, 3, 1, 2)
BACK = (2, 3, 1, 0)


def neighbours():
    dp, ep = lax.axis_index("dp"), lax.axis_index("ep")
    z_hi, core = dp // 2, dp % 2
    x, z_lo, y = ep // 8, (ep // 4) % 2, ep % 4
    z = z_hi * 2 + z_lo
    a = (1 - core) * x + core * y
    b = (1 - core) * y + core * x

    def device(a, b, z):
        px = (1 - core) * a + core * b
        py = (1 - core) * b + core * a
        return ((z // 2) * 2 + core, (px * 2 + z % 2) * 4 + py)

    up = z + 1 - 2 * (z % 2)
    down = (z + 3 + 2 * (z % 2)) % 4
    zp = (1 - core) * up + core * down
    where = {
        "a+": device((a + 1) % 4, b, z),
        "a-": device((a + 3) % 4, b, z),
        "a2": device((a + 2) % 4, b, z),
        "b2": device(a, (b + 2) % 4, z),
        "b+": device(a, (b + 1) % 4, z),
        "b-": device(a, (b + 3) % 4, z),
        "z": device(a, b, zp),
    }
    return where, ep, where["z"][1]


def kernel(
    tokens, ids_in, nums_in, wg_in, wu_in, wd_in, out,
    wg, wu, wd, IN, T, M, X, ZS, YR, PS, G, H, FAR, ADJ, FFR, FA, TRI,
    send, recv, local, wsem,
):
    where, ep, pep = neighbours()
    counter = [0]

    def remote(src, dst, to):
        index = counter[0]
        counter[0] += 1
        return pltpu.make_async_remote_copy(
            src_ref=src, dst_ref=dst, send_sem=send.at[index], recv_sem=recv.at[index],
            device_id=where[to], device_id_type=MESH,
        )

    loads = [
        pltpu.make_async_copy(src.at[e], dst.at[e], wsem.at[k, e])
        for e in range(2)
        for k, (src, dst) in enumerate(((wg_in, wg), (wu_in, wu), (wd_in, wd)))
    ]
    own = pltpu.make_async_copy(tokens, T.at[0, 0], local.at[0])
    tables = [
        pltpu.make_async_copy(ids_in, IN.at[0], local.at[1]),
        pltpu.make_async_copy(nums_in, IN.at[1], local.at[2]),
    ]
    own.start()
    for table in tables:
        table.start()

    mf = [
        remote(M.at[0, 0, 0], M.at[0, 0, 3], "a+"),
        remote(M.at[0, 0, 0], M.at[0, 0, 1], "a-"),
        remote(M.at[0, 0, 0], M.at[0, 0, 2], "a2"),
    ]
    ms = {
        3: remote(M.at[0, 0], M.at[0, 3], "b+"),
        1: remote(M.at[0, 0], M.at[0, 1], "b-"),
        2: remote(M.at[0, 0], M.at[0, 2], "b2"),
    }
    mz = [remote(M.at[0, j], M.at[1, j], "z") for j in range(4)]
    f = {
        (3, 0): remote(T.at[0, 0, 0], T.at[0, 3, 0], "a+"),
        (1, 1): remote(T.at[0, 0, 1], T.at[0, 1, 1], "a+"),
        (2, 0): remote(T.at[0, 3, 0], T.at[0, 2, 0], "a+"),
        (3, 1): remote(T.at[0, 0, 1], T.at[0, 3, 1], "a-"),
        (1, 0): remote(T.at[0, 0, 0], T.at[0, 1, 0], "a-"),
        (2, 1): remote(T.at[0, 3, 1], T.at[0, 2, 1], "a-"),
    }
    s = {}
    for i in range(4):
        s[2, i, 0] = remote(T.at[0, i, 0], T.at[2, i, 0], "b+")
        s[2, i, 1] = remote(T.at[0, i, 1], T.at[2, i, 1], "b-")
        s[1, i, 0] = remote(T.at[2, i, 0], T.at[1, i, 0], "b+")
        s[1, i, 1] = remote(T.at[2, i, 1], T.at[1, i, 1], "b-")
        s[3, i, 1] = remote(T.at[0, i, 1], T.at[3, i, 1], "b+")
        s[3, i, 0] = remote(T.at[0, i, 0], T.at[3, i, 0], "b-")
    zs = {(c, i): remote(ZS.at[c, i], X.at[c, 1, i], "z") for c in range(4) for i in range(4)}
    zr = {(c, i): remote(X.at[c, 1, i], YR.at[c, i], "z") for c in range(4) for i in range(4)}
    far = {}
    adj = {}
    for i in range(4):
        far[i, 0] = remote(T.at[1, i, 0], FAR.at[i, 0], "b+")
        far[i, 1] = remote(T.at[1, i, 1], FAR.at[i, 1], "b-")
        adj[2, i, 0] = remote(T.at[2, i, 0], ADJ.at[1, i, 0], "b-")
        adj[2, i, 1] = remote(T.at[2, i, 1], ADJ.at[0, i, 1], "b+")
        adj[3, i, 0] = remote(T.at[3, i, 0], ADJ.at[0, i, 0], "b+")
        adj[3, i, 1] = remote(T.at[3, i, 1], ADJ.at[1, i, 1], "b-")
    ff = {
        0: remote(T.at[0, 2, 0], FFR.at[0], "a+"),
        1: remote(T.at[0, 2, 1], FFR.at[1], "a-"),
    }
    fa = {
        (1, 0): remote(T.at[0, 1, 0], FA.at[0, 0], "a+"),
        (3, 1): remote(T.at[0, 3, 1], FA.at[0, 1], "a+"),
        (3, 0): remote(T.at[0, 3, 0], FA.at[1, 0], "a-"),
        (1, 1): remote(T.at[0, 1, 1], FA.at[1, 1], "a-"),
    }

    barrier = pltpu.get_barrier_semaphore()
    peers = ("a+", "a-", "a2", "b+", "b-", "b2", "z")
    for name in peers:
        pl.semaphore_signal(barrier, inc=1, device_id=where[name], device_id_type=MESH)

    lane = lax.broadcasted_iota(jnp.int32, (TOK, TOK), 1)
    row = lax.broadcasted_iota(jnp.int32, (TOK, TOK), 0)
    TRI[...] = jnp.where((row < lane) & ((row & 96) == (lane & 96)), 1.0, 0.0).astype(BF)
    for k, table in enumerate(tables):
        table.wait()
        M[0, 0, 0, 8 * k : 8 * k + 8] = jnp.transpose(IN[k].astype(F32)).astype(jnp.int32)
    own.wait()
    for load in loads:
        load.start()

    sub8 = lax.broadcasted_iota(jnp.int32, (8, TOK), 0)
    lane8 = lax.broadcasted_iota(jnp.int32, (8, TOK), 1)
    sub32 = lax.broadcasted_iota(jnp.int32, (CAP, TOK), 0).astype(F32)
    expert = jnp.where(sub8 < 2, 2 * ep + sub8, 2 * pep + sub8 - 2)
    start_slot = ((lane8 & 96) >> 2).astype(F32)

    low = lax.broadcasted_iota(jnp.int32, (16, TOK), 1) < HALF

    def pick(c, i, plane):
        first, second = ((0, 0), (2, 2), (3, 1), (1, 3))[c]
        return jnp.where(low, M[plane, first, i], M[plane, second, (4 - i) % 4])

    def slots_of(table):
        member = jnp.zeros((8, TOK), F32)
        weight = jnp.zeros((8, TOK), jnp.int32)
        for k in range(8):
            hit = table[k : k + 1] == expert
            member = member + jnp.where(hit, 1.0, 0.0)
            weight = weight + jnp.where(hit, table[8 + k : 9 + k], 0)
        before = jnp.dot(member.astype(BF), TRI[...], preferred_element_type=F32)
        code = jnp.where(member > 0.5, start_slot + before, -1.0)
        return code, weight.astype(F32) * (1.0 / 1024.0)

    def weigh(c, i, plane, hits, gate):
        for e in range(2):
            column = jnp.sum(jnp.where(hits[e], gate[e : e + 1], 0.0), axis=1, keepdims=True)
            G[c, e, plane, i] = jnp.broadcast_to(column, (CAP, TOK))

    def pack(c, i):
        code, gate = slots_of(pick(c, i, 0))
        hits = [sub32 == code[r : r + 1] for r in range(4)]
        places = jnp.concatenate([jnp.where(hits[r], 1.0, 0.0) for r in range(4)], axis=0).astype(BF)
        PS[c, i] = places
        for n in range(4):
            cols = slice(512 * n, 512 * n + 512)
            rows = T[c, i, :, :, cols].reshape(TOK, 512)
            packed = jnp.dot(places, rows, preferred_element_type=F32).astype(BF)
            X[c, 0, i, :, :, cols] = packed[:HALF].reshape(2, CAP, 512)
            ZS[c, i, :, :, cols] = packed[HALF:].reshape(2, CAP, 512)
        weigh(c, i, 0, hits, gate)

    def weigh_theirs(c):
        for i in range(4):
            code, gate = slots_of(pick(c, i, 1))
            weigh(c, i, 1, [sub32 == code[r : r + 1] for r in range(2)], gate)

    def gate_up(c, e):
        def step(n, carry):
            cols = pl.ds(pl.multiple_of(n * 256, 256), 256)
            x = X[c, :, :, e].reshape(256, D)
            g = jnp.dot(x, wg[e, :, cols], preferred_element_type=F32)
            u = jnp.dot(x, wu[e, :, cols], preferred_element_type=F32)
            scale = G[c, e].reshape(256, TOK)[:, :1]
            H[:, cols] = (g / (1.0 + jnp.exp(-g)) * u * scale).astype(BF)
            return carry

        lax.fori_loop(0, 3, step, 0)

    def down(c, e):
        def step(n, carry):
            cols = pl.ds(pl.multiple_of(n * 512, 512), 512)
            y = jnp.dot(H[...], wd[e, :, cols], preferred_element_type=F32)
            X[c, :, :, e, :, cols] = y.astype(BF).reshape(2, 4, CAP, 512)
            return carry

        lax.fori_loop(0, 4, step, 0)

    def experts(c, between):
        if c != 3:
            for i in ORDER:
                zs[c, i].wait_recv()
        weigh_theirs(c)
        between = list(between)
        for e in range(2):
            gate_up(c, e)
            if between:
                between.pop(0)()
            down(c, e)
            if between:
                between.pop(0)()
        for task in between:
            task()

    def combine(c, i, extra, target=None):
        for n in range(4):
            cols = slice(512 * n, 512 * n + 512)
            y = jnp.concatenate(
                [X[c, 0, i, :, :, cols].reshape(HALF, 512), YR[c, i, :, :, cols].reshape(HALF, 512)], axis=0
            )
            total = lax.dot_general(PS[c, i], y, (((0,), (0,)), ((), ())), preferred_element_type=F32)
            for part in extra:
                total = total + part[:, :, cols].reshape(TOK, 512).astype(F32)
            if target is None:
                T[c, i, :, :, cols] = total.astype(BF).reshape(2, HALF, 512)
            else:
                target[:, cols] = total.astype(BF)

    def pack_send(c, i):
        pack(c, i)
        zs[c, i].start()

    def near(i):
        for h in range(2):
            s[2, i, h].wait_recv()
            s[1, i, h].start()
        pack_send(2, i)

    def others(i):
        s[3, i, 1].start()
        s[3, i, 0].start()

    def distant(c, i):
        s[c, i, 0].wait_recv()
        s[c, i, 1].wait_recv()
        pack_send(c, i)

    pack(0, 0)
    pl.semaphore_wait(barrier, len(peers))
    for copy in mf:
        copy.start()
    zs[0, 0].start()
    for key in ((3, 0), (3, 1), (1, 1), (1, 0)):
        f[key].start()
    for copy in mf:
        copy.wait_recv()
    for j in (1, 3, 2):
        ms[j].start()
    f[3, 0].wait_recv()
    f[2, 0].start()
    f[3, 1].wait_recv()
    f[2, 1].start()
    pack_send(0, 3)
    mz[0].start()
    for i in (0, 3):
        s[2, i, 0].start()
        s[2, i, 1].start()
    f[1, 0].wait_recv()
    f[1, 1].wait_recv()
    pack_send(0, 1)
    s[2, 1, 0].start()
    s[2, 1, 1].start()
    f[2, 0].wait_recv()
    f[2, 1].wait_recv()
    pack_send(0, 2)
    s[2, 2, 0].start()
    s[2, 2, 1].start()
    for j in (1, 3, 2):
        ms[j].wait_recv()
        mz[j].start()
    near(0)
    near(3)
    others(0)
    near(1)
    others(3)
    for copy in mz:
        copy.wait_recv()
    for load in loads:
        load.wait()

    def last_near():
        near(2)
        others(1)
        others(2)

    experts(0, [last_near])
    distant(1, 0)
    distant(1, 3)
    experts(2, [lambda c=c, i=i: distant(c, i) for c, i in ((1, 1), (1, 2), (3, 0), (3, 3))])
    distant(3, 1)
    distant(3, 2)
    for i in BACK:
        zr[2, i].start()

    def returned(c, i):
        zr[c, i].wait_recv()
        extra = []
        if c == 3:
            far[i, 0].wait_recv()
            far[i, 1].wait_recv()
            extra = [FAR.at[i]]
        combine(c, i, extra)
        for h in range(2):
            (far[i, h] if c == 1 else adj[c, i, h]).start()

    for copy in list(f.values()) + list(s.values()):
        copy.wait_send()
    experts(1, [])
    for i, k in zip(ORDER, BACK):
        zs[3, i].wait_recv()
        zr[1, k].start()
    returned(2, BACK[0])
    returned(2, BACK[1])
    experts(3, [lambda i=i: returned(2, i) for i in BACK[2:]])
    for i in BACK:
        zr[3, i].start()
    for i in BACK:
        returned(1, i)
    for i in BACK:
        returned(3, i)
        zr[0, i].start()
    for i in BACK:
        zr[0, i].wait_recv()
        for c in (2, 3):
            adj[c, i, 0].wait_recv()
            adj[c, i, 1].wait_recv()
        extra = [ADJ.at[0, i], ADJ.at[1, i]]
        if i == 2:
            combine(0, 2, extra)
            ff[0].start()
            ff[1].start()
        if i == 3:
            combine(0, 3, extra)
            fa[3, 0].start()
            fa[3, 1].start()
        if i == 1:
            ff[0].wait_recv()
            ff[1].wait_recv()
            combine(0, 1, extra + [FFR])
            fa[1, 0].start()
            fa[1, 1].start()
        if i == 0:
            for copy in fa.values():
                copy.wait_recv()
            combine(0, 0, extra + [FA.at[0], FA.at[1]], out)

    for copy in [*mz, *mf, *ms.values(), *zs.values(), *zr.values(), *far.values(), *adj.values(), *ff.values(), *fa.values()]:
        copy.wait_send()


COPIES = 10 + 6 + 24 + 16 + 16 + 8 + 16 + 2 + 4


def shards(tokens, expert_ids, gate_nums, w_gate, w_up, w_down):
    anywhere = pl.BlockSpec(memory_space=pl.ANY)
    return pl.pallas_call(
        kernel,
        name="routed_experts",
        out_shape=jax.ShapeDtypeStruct((TOK, D), BF),
        in_specs=[anywhere] * 6,
        out_specs=pl.BlockSpec(memory_space=pltpu.VMEM),
        scratch_shapes=[
            pltpu.VMEM((2, D, FF), BF),
            pltpu.VMEM((2, D, FF), BF),
            pltpu.VMEM((2, FF, D), BF),
            pltpu.VMEM((2, TOK, 8), jnp.int32),
            pltpu.VMEM((4, 4, 2, HALF, D), BF),
            pltpu.VMEM((2, 4, 4, 16, TOK), jnp.int32),
            pltpu.VMEM((4, 2, 4, 2, CAP, D), BF),
            pltpu.VMEM((4, 4, 2, CAP, D), BF),
            pltpu.VMEM((4, 4, 2, CAP, D), BF),
            pltpu.VMEM((4, 4, TOK, TOK), BF),
            pltpu.VMEM((4, 2, 2, 4, CAP, TOK), F32),
            pltpu.VMEM((256, FF), BF),
            pltpu.VMEM((4, 2, HALF, D), BF),
            pltpu.VMEM((2, 4, 2, HALF, D), BF),
            pltpu.VMEM((2, HALF, D), BF),
            pltpu.VMEM((2, 2, HALF, D), BF),
            pltpu.VMEM((TOK, TOK), BF),
            pltpu.SemaphoreType.DMA((COPIES,)),
            pltpu.SemaphoreType.DMA((COPIES,)),
            pltpu.SemaphoreType.DMA((3,)),
            pltpu.SemaphoreType.DMA((3, 2)),
        ],
        compiler_params=pltpu.CompilerParams(
            collective_id=0, has_side_effects=True, vmem_limit_bytes=67043328
        ),
    )(tokens.reshape(2, HALF, D), expert_ids, gate_nums, w_gate, w_up, w_down)


def solution(mesh):
    placed = (
        P(("dp", "ep"), None),
        P(("dp", "ep"), None),
        P(("dp", "ep"), None),
        P("ep", None, None),
        P("ep", None, None),
        P("ep", None, None),
    )
    return jax.shard_map(
        shards, mesh=mesh, in_specs=placed, out_specs=P(("dp", "ep"), None), check_vma=False
    )
```

```python
import jax
import jax.numpy as jnp
from jax import lax
from jax.experimental import pallas as pl
from jax.experimental.pallas import tpu as pltpu
from jax.sharding import PartitionSpec as P

MESH = pl.DeviceIdType.MESH
BF = jnp.bfloat16
F32 = jnp.float32
D = 2048
FF = 768
TOK = 128
HALF = 64
CAP = 32
ORDER = (0, 3, 1, 2)
BACK = (2, 3, 1, 0)


def neighbours():
    dp, ep = lax.axis_index("dp"), lax.axis_index("ep")
    z_hi, core = dp // 2, dp % 2
    x, z_lo, y = ep // 8, (ep // 4) % 2, ep % 4
    z = z_hi * 2 + z_lo
    a = (1 - core) * x + core * y
    b = (1 - core) * y + core * x

    def device(a, b, z):
        px = (1 - core) * a + core * b
        py = (1 - core) * b + core * a
        return ((z // 2) * 2 + core, (px * 2 + z % 2) * 4 + py)

    up = z + 1 - 2 * (z % 2)
    down = (z + 3 + 2 * (z % 2)) % 4
    zp = (1 - core) * up + core * down
    where = {
        "a+": device((a + 1) % 4, b, z),
        "a-": device((a + 3) % 4, b, z),
        "a2": device((a + 2) % 4, b, z),
        "b2": device(a, (b + 2) % 4, z),
        "b+": device(a, (b + 1) % 4, z),
        "b-": device(a, (b + 3) % 4, z),
        "z": device(a, b, zp),
    }
    return where, ep, where["z"][1]


def kernel(
    tokens, ids_in, nums_in, wg_in, wu_in, wd_in, out,
    wg, wu, wd, T, M, X, ZS, YR, PS, G, H, FAR, ADJ, FFR, FA, TRI,
    send, recv, local, wsem,
):
    where, ep, pep = neighbours()
    counter = [0]

    def remote(src, dst, to):
        index = counter[0]
        counter[0] += 1
        return pltpu.make_async_remote_copy(
            src_ref=src, dst_ref=dst, send_sem=send.at[index], recv_sem=recv.at[index],
            device_id=where[to], device_id_type=MESH,
        )

    loads = [
        pltpu.make_async_copy(src.at[e], dst.at[e], wsem.at[k, e])
        for e in range(2)
        for k, (src, dst) in enumerate(((wg_in, wg), (wu_in, wu), (wd_in, wd)))
    ]
    own = pltpu.make_async_copy(tokens, T.at[0, 0], local.at[0])
    tables = [
        pltpu.make_async_copy(ids_in, M.at[0, 0, 0, pl.ds(0, 8)], local.at[1]),
        pltpu.make_async_copy(nums_in, M.at[0, 0, 0, pl.ds(8, 8)], local.at[2]),
    ]
    own.start()
    for table in tables:
        table.start()

    mf = [
        remote(M.at[0, 0, 0], M.at[0, 0, 3], "a+"),
        remote(M.at[0, 0, 0], M.at[0, 0, 1], "a-"),
        remote(M.at[0, 0, 0], M.at[0, 0, 2], "a2"),
    ]
    ms = {
        3: remote(M.at[0, 0], M.at[0, 3], "b+"),
        1: remote(M.at[0, 0], M.at[0, 1], "b-"),
        2: remote(M.at[0, 0], M.at[0, 2], "b2"),
    }
    mz = [remote(M.at[0, j], M.at[1, j], "z") for j in range(4)]
    f = {
        (3, 0): remote(T.at[0, 0, 0], T.at[0, 3, 0], "a+"),
        (1, 1): remote(T.at[0, 0, 1], T.at[0, 1, 1], "a+"),
        (2, 0): remote(T.at[0, 3, 0], T.at[0, 2, 0], "a+"),
        (3, 1): remote(T.at[0, 0, 1], T.at[0, 3, 1], "a-"),
        (1, 0): remote(T.at[0, 0, 0], T.at[0, 1, 0], "a-"),
        (2, 1): remote(T.at[0, 3, 1], T.at[0, 2, 1], "a-"),
    }
    s = {}
    for i in range(4):
        s[2, i, 0] = remote(T.at[0, i, 0], T.at[2, i, 0], "b+")
        s[2, i, 1] = remote(T.at[0, i, 1], T.at[2, i, 1], "b-")
        s[1, i, 0] = remote(T.at[2, i, 0], T.at[1, i, 0], "b+")
        s[1, i, 1] = remote(T.at[2, i, 1], T.at[1, i, 1], "b-")
        s[3, i, 1] = remote(T.at[0, i, 1], T.at[3, i, 1], "b+")
        s[3, i, 0] = remote(T.at[0, i, 0], T.at[3, i, 0], "b-")
    zs = {(c, i): remote(ZS.at[c, i], X.at[c, 1, i], "z") for c in range(4) for i in range(4)}
    zr = {(c, i): remote(X.at[c, 1, i], YR.at[c, i], "z") for c in range(4) for i in range(4)}
    far = {}
    adj = {}
    for i in range(4):
        far[i, 0] = remote(T.at[1, i, 0], FAR.at[i, 0], "b+")
        far[i, 1] = remote(T.at[1, i, 1], FAR.at[i, 1], "b-")
        adj[2, i, 0] = remote(T.at[2, i, 0], ADJ.at[1, i, 0], "b-")
        adj[2, i, 1] = remote(T.at[2, i, 1], ADJ.at[0, i, 1], "b+")
        adj[3, i, 0] = remote(T.at[3, i, 0], ADJ.at[0, i, 0], "b+")
        adj[3, i, 1] = remote(T.at[3, i, 1], ADJ.at[1, i, 1], "b-")
    ff = {
        0: remote(T.at[0, 2, 0], FFR.at[0], "a+"),
        1: remote(T.at[0, 2, 1], FFR.at[1], "a-"),
    }
    fa = {
        (1, 0): remote(T.at[0, 1, 0], FA.at[0, 0], "a+"),
        (3, 1): remote(T.at[0, 3, 1], FA.at[0, 1], "a+"),
        (3, 0): remote(T.at[0, 3, 0], FA.at[1, 0], "a-"),
        (1, 1): remote(T.at[0, 1, 1], FA.at[1, 1], "a-"),
    }

    barrier = pltpu.get_barrier_semaphore()
    peers = ("a+", "a-", "a2", "b+", "b-", "b2", "z")
    for name in peers:
        pl.semaphore_signal(barrier, inc=1, device_id=where[name], device_id_type=MESH)

    lane = lax.broadcasted_iota(jnp.int32, (TOK, TOK), 1)
    row = lax.broadcasted_iota(jnp.int32, (TOK, TOK), 0)
    TRI[...] = jnp.where((row < lane) & ((row & 96) == (lane & 96)), 1.0, 0.0).astype(BF)
    for table in tables:
        table.wait()
    own.wait()
    for load in loads:
        load.start()

    sub8 = lax.broadcasted_iota(jnp.int32, (8, TOK), 0)
    lane8 = lax.broadcasted_iota(jnp.int32, (8, TOK), 1)
    sub32 = lax.broadcasted_iota(jnp.int32, (CAP, TOK), 0).astype(F32)
    expert = jnp.where(sub8 < 2, 2 * ep + sub8, 2 * pep + sub8 - 2)
    start_slot = ((lane8 & 96) >> 2).astype(F32)

    low = lax.broadcasted_iota(jnp.int32, (16, TOK), 1) < HALF

    def pick(c, i, plane):
        first, second = ((0, 0), (2, 2), (3, 1), (1, 3))[c]
        return jnp.where(low, M[plane, first, i], M[plane, second, (4 - i) % 4])

    def slots_of(table):
        member = jnp.zeros((8, TOK), F32)
        weight = jnp.zeros((8, TOK), jnp.int32)
        for k in range(8):
            hit = table[k : k + 1] == expert
            member = member + jnp.where(hit, 1.0, 0.0)
            weight = weight + jnp.where(hit, table[8 + k : 9 + k], 0)
        before = jnp.dot(member.astype(BF), TRI[...], preferred_element_type=F32)
        code = jnp.where(member > 0.5, start_slot + before, -1.0)
        return code, weight.astype(F32) * (1.0 / 1024.0)

    def weigh(c, i, plane, hits, gate):
        for e in range(2):
            column = jnp.sum(jnp.where(hits[e], gate[e : e + 1], 0.0), axis=1, keepdims=True)
            G[c, e, plane, i] = jnp.broadcast_to(column, (CAP, TOK))

    def pack(c, i):
        code, gate = slots_of(pick(c, i, 0))
        hits = [sub32 == code[r : r + 1] for r in range(4)]
        places = jnp.concatenate([jnp.where(hits[r], 1.0, 0.0) for r in range(4)], axis=0).astype(BF)
        PS[c, i] = places
        for n in range(4):
            cols = slice(512 * n, 512 * n + 512)
            rows = T[c, i, :, :, cols].reshape(TOK, 512)
            packed = jnp.dot(places, rows, preferred_element_type=F32).astype(BF)
            X[c, 0, i, :, :, cols] = packed[:HALF].reshape(2, CAP, 512)
            ZS[c, i, :, :, cols] = packed[HALF:].reshape(2, CAP, 512)
        weigh(c, i, 0, hits, gate)

    def weigh_theirs(c):
        for i in range(4):
            code, gate = slots_of(pick(c, i, 1))
            weigh(c, i, 1, [sub32 == code[r : r + 1] for r in range(2)], gate)

    def gate_up(c, e, n):
        cols = slice(256 * n, 256 * n + 256) if isinstance(n, int) else pl.ds(pl.multiple_of(n * 256, 256), 256)
        x = X[c, :, :, e].reshape(256, D)
        g = jnp.dot(x, wg[e, :, cols], preferred_element_type=F32)
        u = jnp.dot(x, wu[e, :, cols], preferred_element_type=F32)
        scale = G[c, e].reshape(256, TOK)[:, :1]
        H[:, cols] = (g / (1.0 + jnp.exp(-g)) * u * scale).astype(BF)

    def down(c, e, n):
        cols = pl.ds(pl.multiple_of(n * 512, 512), 512)
        y = jnp.dot(H[...], wd[e, :, cols], preferred_element_type=F32)
        X[c, :, :, e, :, cols] = y.astype(BF).reshape(2, 4, CAP, 512)

    def loop(low, high, step):
        def body(n, carry):
            step(n)
            return carry

        lax.fori_loop(low, high, body, 0)

    def arrived(c):
        for i in ORDER:
            zs[c, i].wait_recv()
        weigh_theirs(c)

    def fine(c, e):
        return [lambda n=n: gate_up(c, e, n) for n in range(3)] + [
            lambda n=n: loop(n, n + 2, lambda m: down(c, e, m)) for n in (0, 2)
        ]

    def coarse(c, e):
        return [
            lambda: loop(0, 3, lambda n: gate_up(c, e, n)),
            lambda: loop(0, 4, lambda m: down(c, e, m)),
        ]

    def run(steps, count=None):
        for _ in range(len(steps) if count is None else count):
            steps.pop(0)()

    def combine(c, i, extra, target=None):
        for n in range(4):
            cols = slice(512 * n, 512 * n + 512)
            y = jnp.concatenate(
                [X[c, 0, i, :, :, cols].reshape(HALF, 512), YR[c, i, :, :, cols].reshape(HALF, 512)], axis=0
            )
            total = lax.dot_general(PS[c, i], y, (((0,), (0,)), ((), ())), preferred_element_type=F32)
            for part in extra:
                total = total + part[:, :, cols].reshape(TOK, 512).astype(F32)
            if target is None:
                T[c, i, :, :, cols] = total.astype(BF).reshape(2, HALF, 512)
            else:
                target[:, cols] = total.astype(BF)

    def pack_send(c, i):
        pack(c, i)
        zs[c, i].start()

    def near(i):
        for h in range(2):
            s[2, i, h].wait_recv()
            s[1, i, h].start()
        pack_send(2, i)

    def others(i):
        s[3, i, 1].start()
        s[3, i, 0].start()

    def distant(c, i):
        s[c, i, 0].wait_recv()
        s[c, i, 1].wait_recv()
        pack_send(c, i)

    def returned(c, i):
        zr[c, i].wait_recv()
        extra = []
        if c == 3:
            far[i, 0].wait_recv()
            far[i, 1].wait_recv()
            extra = [FAR.at[i]]
        combine(c, i, extra)
        for h in range(2):
            (far[i, h] if c == 1 else adj[c, i, h]).start()

    def pack_send(c, i):
        pack(c, i)
        zs[c, i].start()

    def near(i):
        for h in range(2):
            s[2, i, h].wait_recv()
            s[1, i, h].start()
        pack_send(2, i)

    def others(i):
        s[3, i, 1].start()
        s[3, i, 0].start()

    def distant(c, i):
        s[c, i, 0].wait_recv()
        s[c, i, 1].wait_recv()
        pack_send(c, i)

    pack(0, 0)
    pl.semaphore_wait(barrier, len(peers))
    f[3, 0].start()
    f[3, 1].start()
    for copy in mf:
        copy.start()
    zs[0, 0].start()
    f[1, 1].start()
    f[1, 0].start()
    f[3, 0].wait_recv()
    f[2, 0].start()
    f[3, 1].wait_recv()
    f[2, 1].start()
    for copy in mf:
        copy.wait_recv()
    for j in (1, 3, 2):
        ms[j].start()
    pack_send(0, 3)
    mz[0].start()
    f[1, 0].wait_recv()
    f[1, 1].wait_recv()
    for i in (0, 3, 1):
        s[2, i, 0].start()
        s[2, i, 1].start()
    pack_send(0, 1)
    f[2, 0].wait_recv()
    f[2, 1].wait_recv()
    pack_send(0, 2)
    s[2, 2, 0].start()
    s[2, 2, 1].start()
    for j in (1, 3, 2):
        ms[j].wait_recv()
        mz[j].start()
    near(0)
    near(3)
    others(0)
    near(1)
    others(3)
    near(2)
    others(1)
    others(2)
    distant(1, 0)
    for copy in mz:
        copy.wait_recv()
    for load in loads:
        load.wait()
    arrived(0)
    first = fine(0, 0)
    run(first, 2)
    distant(1, 3)
    run(first, 2)
    distant(3, 0)
    run(first)
    distant(1, 1)
    arrived(2)
    second = fine(2, 0) + fine(2, 1)
    run(second, 2)
    distant(3, 3)
    run(second, 3)
    distant(1, 2)
    run(second, 2)
    distant(3, 1)
    run(second, 2)
    distant(3, 2)
    run(second)
    for i in BACK:
        zr[2, i].start()
    for copy in list(f.values()) + list(s.values()):
        copy.wait_send()
    arrived(1)
    run(coarse(1, 0) + coarse(1, 1))
    for i, k in zip(ORDER, BACK):
        zs[3, i].wait_recv()
        zr[1, k].start()
    weigh_theirs(3)
    returned(2, 2)
    third = coarse(3, 0) + coarse(3, 1)
    run(third, 1)
    returned(2, 3)
    run(third, 1)
    returned(2, 1)
    run(third, 1)
    returned(2, 0)
    run(third)
    zr[3, 2].start()
    zr[3, 3].start()
    returned(1, 2)
    last = coarse(0, 1)
    run(last, 1)
    returned(1, 3)
    run(last)
    returned(1, 1)
    returned(1, 0)
    zr[0, 2].start()
    zr[3, 1].start()

    def finish(i, extra, target=None):
        zr[0, i].wait_recv()
        for c in (2, 3):
            adj[c, i, 0].wait_recv()
            adj[c, i, 1].wait_recv()
        combine(0, i, [ADJ.at[0, i], ADJ.at[1, i]] + extra, target)

    returned(3, 2)
    zr[0, 3].start()
    returned(3, 3)
    zr[3, 0].start()
    finish(2, [])
    ff[0].start()
    ff[1].start()
    zr[0, 1].start()
    returned(3, 1)
    zr[0, 0].start()
    finish(3, [])
    fa[3, 0].start()
    fa[3, 1].start()
    returned(3, 0)
    ff[0].wait_recv()
    ff[1].wait_recv()
    finish(1, [FFR])
    fa[1, 0].start()
    fa[1, 1].start()
    for copy in fa.values():
        copy.wait_recv()
    finish(0, [FA.at[0], FA.at[1]], out)

    for copy in [*mz, *mf, *ms.values(), *zs.values(), *zr.values(), *far.values(), *adj.values(), *ff.values(), *fa.values()]:
        copy.wait_send()


COPIES = 10 + 6 + 24 + 16 + 16 + 8 + 16 + 2 + 4


def shards(tokens, expert_ids, gate_nums, w_gate, w_up, w_down):
    anywhere = pl.BlockSpec(memory_space=pl.ANY)
    return pl.pallas_call(
        kernel,
        name="routed_experts",
        out_shape=pltpu.VMEM((TOK, D), BF),
        in_specs=[anywhere] * 6,
        out_specs=pl.BlockSpec(memory_space=pltpu.VMEM),
        scratch_shapes=[
            pltpu.VMEM((2, D, FF), BF),
            pltpu.VMEM((2, D, FF), BF),
            pltpu.VMEM((2, FF, D), BF),
            pltpu.VMEM((4, 4, 2, HALF, D), BF),
            pltpu.VMEM((2, 4, 4, 16, TOK), jnp.int32),
            pltpu.VMEM((4, 2, 4, 2, CAP, D), BF),
            pltpu.VMEM((4, 4, 2, CAP, D), BF),
            pltpu.VMEM((4, 4, 2, CAP, D), BF),
            pltpu.VMEM((4, 4, TOK, TOK), BF),
            pltpu.VMEM((4, 2, 2, 4, CAP, TOK), F32),
            pltpu.VMEM((256, FF), BF),
            pltpu.VMEM((4, 2, HALF, D), BF),
            pltpu.VMEM((2, 4, 2, HALF, D), BF),
            pltpu.VMEM((2, HALF, D), BF),
            pltpu.VMEM((2, 2, HALF, D), BF),
            pltpu.VMEM((TOK, TOK), BF),
            pltpu.SemaphoreType.DMA((COPIES,)),
            pltpu.SemaphoreType.DMA((COPIES,)),
            pltpu.SemaphoreType.DMA((3,)),
            pltpu.SemaphoreType.DMA((3, 2)),
        ],
        compiler_params=pltpu.CompilerParams(
            collective_id=0, has_side_effects=True, vmem_limit_bytes=62 * 1024 * 1024
        ),
    )(tokens.reshape(2, HALF, D), expert_ids.T, gate_nums.T, w_gate, w_up, w_down)


def solution(mesh):
    placed = (
        P(("dp", "ep"), None),
        P(("dp", "ep"), None),
        P(("dp", "ep"), None),
        P("ep", None, None),
        P("ep", None, None),
        P("ep", None, None),
    )
    return jax.shard_map(
        shards, mesh=mesh, in_specs=placed, out_specs=P(("dp", "ep"), None), check_vma=False
    )
```

```python
import jax
import jax.numpy as jnp
from jax import lax
from jax.experimental import pallas as pl
from jax.experimental.pallas import tpu as pltpu
from jax.sharding import PartitionSpec as P

MESH = pl.DeviceIdType.MESH
BF = jnp.bfloat16
F32 = jnp.float32
D = 2048
FF = 768
TOK = 128
HALF = 64
CAP = 32
ORDER = (0, 3, 1, 2)
BACK = (2, 3, 1, 0)


def neighbours():
    dp, ep = lax.axis_index("dp"), lax.axis_index("ep")
    z_hi, core = dp // 2, dp % 2
    x, z_lo, y = ep // 8, (ep // 4) % 2, ep % 4
    z = z_hi * 2 + z_lo
    a = (1 - core) * x + core * y
    b = (1 - core) * y + core * x

    def device(a, b, z):
        px = (1 - core) * a + core * b
        py = (1 - core) * b + core * a
        return ((z // 2) * 2 + core, (px * 2 + z % 2) * 4 + py)

    up = z + 1 - 2 * (z % 2)
    down = (z + 3 + 2 * (z % 2)) % 4
    zp = (1 - core) * up + core * down
    where = {
        "a+": device((a + 1) % 4, b, z),
        "a-": device((a + 3) % 4, b, z),
        "a2": device((a + 2) % 4, b, z),
        "b2": device(a, (b + 2) % 4, z),
        "b+": device(a, (b + 1) % 4, z),
        "b-": device(a, (b + 3) % 4, z),
        "z": device(a, b, zp),
    }
    return where, ep, where["z"][1]


def kernel(
    tokens, ids_in, nums_in, wg_in, wu_in, wd_in, out,
    wg, wu, wd, T, M, X, ZS, YR, PS, G, H, FAR, ADJ, FFR, FA, TRI,
    send, recv, local, wsem,
):
    where, ep, pep = neighbours()
    counter = [0]

    def remote(src, dst, to):
        index = counter[0]
        counter[0] += 1
        return pltpu.make_async_remote_copy(
            src_ref=src, dst_ref=dst, send_sem=send.at[index], recv_sem=recv.at[index],
            device_id=where[to], device_id_type=MESH,
        )

    loads = [
        pltpu.make_async_copy(src.at[e], dst.at[e], wsem.at[k, e])
        for e in range(2)
        for k, (src, dst) in enumerate(((wg_in, wg), (wu_in, wu), (wd_in, wd)))
    ]
    own = pltpu.make_async_copy(tokens, T.at[0, 0], local.at[0])
    tables = [
        pltpu.make_async_copy(ids_in, M.at[0, 0, 0, pl.ds(0, 8)], local.at[1]),
        pltpu.make_async_copy(nums_in, M.at[0, 0, 0, pl.ds(8, 8)], local.at[2]),
    ]
    own.start()
    for table in tables:
        table.start()

    mf = [
        remote(M.at[0, 0, 0], M.at[0, 0, 3], "a+"),
        remote(M.at[0, 0, 0], M.at[0, 0, 1], "a-"),
        remote(M.at[0, 0, 0], M.at[0, 0, 2], "a2"),
    ]
    ms = {
        3: remote(M.at[0, 0], M.at[0, 3], "b+"),
        1: remote(M.at[0, 0], M.at[0, 1], "b-"),
        2: remote(M.at[0, 0], M.at[0, 2], "b2"),
    }
    mz = [remote(M.at[0, j], M.at[1, j], "z") for j in range(4)]
    f = {}
    for q in range(2):
        part = pl.ds(32 * q, 32)
        f[3, 0, q] = remote(T.at[0, 0, 0, part], T.at[0, 3, 0, part], "a+")
        f[1, 1, q] = remote(T.at[0, 0, 1, part], T.at[0, 1, 1, part], "a+")
        f[2, 0, q] = remote(T.at[0, 3, 0, part], T.at[0, 2, 0, part], "a+")
        f[3, 1, q] = remote(T.at[0, 0, 1, part], T.at[0, 3, 1, part], "a-")
        f[1, 0, q] = remote(T.at[0, 0, 0, part], T.at[0, 1, 0, part], "a-")
        f[2, 1, q] = remote(T.at[0, 3, 1, part], T.at[0, 2, 1, part], "a-")
    s = {}
    for i in range(4):
        s[2, i, 0] = remote(T.at[0, i, 0], T.at[2, i, 0], "b+")
        s[2, i, 1] = remote(T.at[0, i, 1], T.at[2, i, 1], "b-")
        s[1, i, 0] = remote(T.at[2, i, 0], T.at[1, i, 0], "b+")
        s[1, i, 1] = remote(T.at[2, i, 1], T.at[1, i, 1], "b-")
        s[3, i, 1] = remote(T.at[0, i, 1], T.at[3, i, 1], "b+")
        s[3, i, 0] = remote(T.at[0, i, 0], T.at[3, i, 0], "b-")
    zs = {(c, i): remote(ZS.at[c, i], X.at[c, 1, i], "z") for c in range(4) for i in range(4) if c or not i}
    zq = {}
    for i in range(1, 4):
        for q in range(2):
            part = pl.ds(16 * q, 16)
            zq[i, q] = remote(ZS.at[0, i, :, part], X.at[0, 1, i, :, part], "z")
    zr = {(c, i): remote(X.at[c, 1, i], YR.at[c, i], "z") for c in range(4) for i in range(4) if (c, i) != (0, 1)}
    zl = []
    for q in range(2):
        part = pl.ds(16 * q, 16)
        zl.append(remote(X.at[0, 1, 1, :, part], YR.at[0, 1, :, part], "z"))
    far = {}
    adj = {}
    for i in range(4):
        far[i, 0] = remote(T.at[1, i, 0], FAR.at[i, 0], "b+")
        far[i, 1] = remote(T.at[1, i, 1], FAR.at[i, 1], "b-")
        adj[2, i, 0] = remote(T.at[2, i, 0], ADJ.at[1, i, 0], "b-")
        adj[2, i, 1] = remote(T.at[2, i, 1], ADJ.at[0, i, 1], "b+")
        adj[3, i, 0] = remote(T.at[3, i, 0], ADJ.at[0, i, 0], "b+")
        adj[3, i, 1] = remote(T.at[3, i, 1], ADJ.at[1, i, 1], "b-")
    ff = {
        0: remote(T.at[0, 2, 0], FFR.at[0], "a+"),
        1: remote(T.at[0, 2, 1], FFR.at[1], "a-"),
    }
    fa = {
        (3, 1): remote(T.at[0, 3, 1], FA.at[0, 1], "a+"),
        (3, 0): remote(T.at[0, 3, 0], FA.at[1, 0], "a-"),
    }
    for q in range(2):
        part = pl.ds(32 * q, 32)
        fa[1, 0, q] = remote(T.at[0, 1, 0, part], FA.at[0, 0, part], "a+")
        fa[1, 1, q] = remote(T.at[0, 1, 1, part], FA.at[1, 1, part], "a-")

    barrier = pltpu.get_barrier_semaphore()
    peers = ("a+", "a-", "a2", "b+", "b-", "b2", "z")
    for name in peers:
        pl.semaphore_signal(barrier, inc=1, device_id=where[name], device_id_type=MESH)

    lane = lax.broadcasted_iota(jnp.int32, (TOK, TOK), 1)
    row = lax.broadcasted_iota(jnp.int32, (TOK, TOK), 0)
    TRI[...] = jnp.where((row < lane) & ((row & 96) == (lane & 96)), 1.0, 0.0).astype(BF)
    for table in tables:
        table.wait()
    own.wait()
    for load in loads:
        load.start()

    sub8 = lax.broadcasted_iota(jnp.int32, (8, TOK), 0)
    lane8 = lax.broadcasted_iota(jnp.int32, (8, TOK), 1)
    sub32 = lax.broadcasted_iota(jnp.int32, (CAP, TOK), 0).astype(F32)
    expert = jnp.where(sub8 < 2, 2 * ep + sub8, 2 * pep + sub8 - 2)
    start_slot = (((lane8 & 32) >> 1) + ((lane8 & 64) >> 3)).astype(F32)

    low = lax.broadcasted_iota(jnp.int32, (16, TOK), 1) < HALF

    def pick(c, i, plane):
        first, second = ((0, 0), (2, 2), (3, 1), (1, 3))[c]
        return jnp.where(low, M[plane, first, i], M[plane, second, (4 - i) % 4])

    def slots_of(table):
        member = jnp.zeros((8, TOK), F32)
        weight = jnp.zeros((8, TOK), jnp.int32)
        for k in range(8):
            hit = table[k : k + 1] == expert
            member = member + jnp.where(hit, 1.0, 0.0)
            weight = weight + jnp.where(hit, table[8 + k : 9 + k], 0)
        before = jnp.dot(member.astype(BF), TRI[...], preferred_element_type=F32)
        code = jnp.where(member > 0.5, start_slot + before, -1.0)
        return code, weight.astype(F32) * (1.0 / 1024.0)

    def weigh(c, i, plane, hits, gate):
        for e in range(2):
            column = jnp.sum(jnp.where(hits[e], gate[e : e + 1], 0.0), axis=1, keepdims=True)
            G[c, e, plane, i] = jnp.broadcast_to(column, (CAP, TOK))

    def place(c, i):
        code, gate = slots_of(pick(c, i, 0))
        hits = [sub32 == code[r : r + 1] for r in range(4)]
        places = jnp.concatenate([jnp.where(hits[r], 1.0, 0.0) for r in range(4)], axis=0).astype(BF)
        PS[c, i] = places
        weigh(c, i, 0, hits, gate)
        return places

    def pack(c, i):
        places = place(c, i)
        for n in range(4):
            cols = slice(512 * n, 512 * n + 512)
            rows = T[c, i, :, :, cols].reshape(TOK, 512)
            packed = jnp.dot(places, rows, preferred_element_type=F32).astype(BF)
            X[c, 0, i, :, :, cols] = packed[:HALF].reshape(2, CAP, 512)
            ZS[c, i, :, :, cols] = packed[HALF:].reshape(2, CAP, 512)

    def pack_quarter(i, q):
        part, own = slice(16 * q, 16 * q + 16), slice(32 * q, 32 * q + 32)
        places = jnp.concatenate([PS[0, i, 32 * r + 16 * q : 32 * r + 16 * q + 16] for r in range(4)], axis=0)
        for n in range(4):
            cols = slice(512 * n, 512 * n + 512)
            first, second = T[0, i, 0, own, cols], T[0, i, 1, own, cols]
            rows = jnp.concatenate([first, first, second, second], axis=0)
            packed = jnp.dot(places, rows, preferred_element_type=F32).astype(BF)
            X[0, 0, i, :, part, cols] = packed[:32].reshape(2, 16, 512)
            ZS[0, i, :, part, cols] = packed[32:].reshape(2, 16, 512)
        zq[i, q].start()

    def weigh_theirs(c):
        for i in range(4):
            code, gate = slots_of(pick(c, i, 1))
            weigh(c, i, 1, [sub32 == code[r : r + 1] for r in range(2)], gate)

    def gate_up(c, e, n):
        cols = slice(256 * n, 256 * n + 256) if isinstance(n, int) else pl.ds(pl.multiple_of(n * 256, 256), 256)
        x = X[c, :, :, e].reshape(256, D)
        g = jnp.dot(x, wg[e, :, cols], preferred_element_type=F32)
        u = jnp.dot(x, wu[e, :, cols], preferred_element_type=F32)
        scale = G[c, e].reshape(256, TOK)[:, :1]
        H[:, cols] = (g / (1.0 + jnp.exp(-g)) * u * scale).astype(BF)

    def down(c, e, n):
        cols = pl.ds(pl.multiple_of(n * 512, 512), 512)
        y = jnp.dot(H[...], wd[e, :, cols], preferred_element_type=F32)
        X[c, :, :, e, :, cols] = y.astype(BF).reshape(2, 4, CAP, 512)

    def loop(low, high, step):
        def body(n, carry):
            step(n)
            return carry

        lax.fori_loop(low, high, body, 0)

    def arrived(c):
        for copy in [zs[0, 0], *zq.values()] if c == 0 else [zs[c, i] for i in ORDER]:
            copy.wait_recv()
        weigh_theirs(c)

    def fine(c, e):
        return [lambda n=n: gate_up(c, e, n) for n in range(3)] + [
            lambda n=n: loop(n, n + 2, lambda m: down(c, e, m)) for n in (0, 2)
        ]

    def coarse(c, e):
        return [
            lambda: loop(0, 3, lambda n: gate_up(c, e, n)),
            lambda: loop(0, 4, lambda m: down(c, e, m)),
        ]

    def run(steps, count=None):
        for _ in range(len(steps) if count is None else count):
            steps.pop(0)()

    def combine(c, i, extra, target=None):
        for n in range(4):
            cols = slice(512 * n, 512 * n + 512)
            y = jnp.concatenate(
                [X[c, 0, i, :, :, cols].reshape(HALF, 512), YR[c, i, :, :, cols].reshape(HALF, 512)], axis=0
            )
            total = lax.dot_general(PS[c, i], y, (((0,), (0,)), ((), ())), preferred_element_type=F32)
            for part in extra:
                total = total + part[:, :, cols].reshape(TOK, 512).astype(F32)
            if target is None:
                T[c, i, :, :, cols] = total.astype(BF).reshape(2, HALF, 512)
            else:
                target[:, cols] = total.astype(BF)

    def pack_send(c, i):
        pack(c, i)
        zs[c, i].start()

    def near(i):
        for h in range(2):
            s[2, i, h].wait_recv()
            s[1, i, h].start()
        pack_send(2, i)

    def others(i):
        s[3, i, 1].start()
        s[3, i, 0].start()

    def distant(c, i):
        s[c, i, 0].wait_recv()
        s[c, i, 1].wait_recv()
        pack_send(c, i)

    def returned(c, i):
        zr[c, i].wait_recv()
        extra = []
        if c == 3:
            far[i, 0].wait_recv()
            far[i, 1].wait_recv()
            extra = [FAR.at[i]]
        combine(c, i, extra)
        for h in range(2):
            (far[i, h] if c == 1 else adj[c, i, h]).start()

    def pack_send(c, i):
        pack(c, i)
        zs[c, i].start()

    def near(i):
        for h in range(2):
            s[2, i, h].wait_recv()
            s[1, i, h].start()
        pack_send(2, i)

    def others(i):
        s[3, i, 1].start()
        s[3, i, 0].start()

    def distant(c, i):
        s[c, i, 0].wait_recv()
        s[c, i, 1].wait_recv()
        pack_send(c, i)

    pack(0, 0)
    pl.semaphore_wait(barrier, len(peers))
    for q in range(2):
        f[3, 0, q].start()
        f[3, 1, q].start()
        if q == 0:
            for copy in mf:
                copy.start()
            zs[0, 0].start()
    for q in range(2):
        f[1, 1, q].start()
        f[1, 0, q].start()
    for q in range(2):
        for h in range(2):
            f[3, h, q].wait_recv()
            f[2, h, q].start()
        if q == 0:
            for copy in mf:
                copy.wait_recv()
            place(0, 3)
            for j in (1, 3, 2):
                ms[j].start()
        pack_quarter(3, q)
    place(0, 1)
    for q in range(2):
        for h in range(2):
            f[1, h, q].wait_recv()
        for i in ((), (0, 3, 1))[q]:
            s[2, i, 0].start()
            s[2, i, 1].start()
        pack_quarter(1, q)
    mz[0].start()
    for j in (1, 3, 2):
        ms[j].wait_recv()
        mz[j].start()
    place(0, 2)
    for q in range(2):
        for h in range(2):
            f[2, h, q].wait_recv()
        pack_quarter(2, q)
    s[2, 2, 0].start()
    s[2, 2, 1].start()
    near(0)
    near(3)
    others(0)
    near(1)
    others(3)
    near(2)
    others(1)
    others(2)
    distant(1, 0)
    for copy in mz:
        copy.wait_recv()
    for load in loads:
        load.wait()
    arrived(0)
    first = fine(0, 0)
    run(first, 2)
    distant(1, 3)
    run(first, 2)
    distant(3, 0)
    run(first)
    distant(1, 1)
    arrived(2)
    second = fine(2, 0) + fine(2, 1)
    run(second, 2)
    distant(3, 3)
    run(second, 3)
    distant(1, 2)
    run(second, 2)
    distant(3, 1)
    run(second, 2)
    distant(3, 2)
    run(second)
    for i in BACK:
        zr[2, i].start()
    for copy in list(f.values()) + list(s.values()):
        copy.wait_send()
    arrived(1)
    run(coarse(1, 0) + coarse(1, 1))
    for i, k in zip(ORDER, BACK):
        zs[3, i].wait_recv()
        zr[1, k].start()
    weigh_theirs(3)
    returned(2, 2)
    third = coarse(3, 0) + coarse(3, 1)
    run(third, 1)
    returned(2, 3)
    run(third, 1)
    returned(2, 1)
    run(third, 1)
    returned(2, 0)
    run(third)
    zr[3, 2].start()
    zr[3, 3].start()
    returned(1, 2)
    last = coarse(0, 1)
    run(last, 1)
    returned(1, 3)
    run(last)
    returned(1, 1)
    returned(1, 0)
    zr[0, 2].start()
    zr[3, 1].start()

    def finish(i, extra, target=None):
        zr[0, i].wait_recv()
        for c in (2, 3):
            adj[c, i, 0].wait_recv()
            adj[c, i, 1].wait_recv()
        combine(0, i, [ADJ.at[0, i], ADJ.at[1, i]] + extra, target)

    returned(3, 2)
    zr[0, 3].start()
    returned(3, 3)
    zr[3, 0].start()
    finish(2, [])
    ff[0].start()
    ff[1].start()
    zl[0].start()
    zl[1].start()
    returned(3, 1)
    zr[0, 0].start()
    finish(3, [])
    fa[3, 0].start()
    fa[3, 1].start()
    returned(3, 0)
    for c in (2, 3):
        for h in range(2):
            adj[c, 1, h].wait_recv()
    ff[0].wait_recv()
    ff[1].wait_recv()
    for q in range(2):
        zl[q].wait_recv()
        part, own = slice(16 * q, 16 * q + 16), slice(32 * q, 32 * q + 32)
        places = jnp.concatenate([PS[0, 1, 32 * r + 16 * q : 32 * r + 16 * q + 16] for r in range(4)], axis=0)
        for n in range(4):
            cols = slice(512 * n, 512 * n + 512)
            y = jnp.concatenate(
                [X[0, 0, 1, :, part, cols].reshape(32, 512), YR[0, 1, :, part, cols].reshape(32, 512)], axis=0
            )
            total = lax.dot_general(places, y, (((0,), (0,)), ((), ())), preferred_element_type=F32)
            for h in range(2):
                rows = total[64 * h + 32 * q : 64 * h + 32 * q + 32]
                for ref in (ADJ.at[0, 1, h], ADJ.at[1, 1, h], FFR.at[h]):
                    rows = rows + ref[own, cols].astype(F32)
                T[0, 1, h, own, cols] = rows.astype(BF)
        fa[1, 0, q].start()
        fa[1, 1, q].start()
    for copy in fa.values():
        copy.wait_recv()
    finish(0, [FA.at[0], FA.at[1]], out)

    for copy in [*mz, *mf, *ms.values(), *zs.values(), *zq.values(), *zl, *zr.values(), *far.values(), *adj.values(), *ff.values(), *fa.values()]:
        copy.wait_send()


COPIES = 10 + 12 + 24 + 13 + 6 + 17 + 8 + 16 + 2 + 6


def shards(tokens, expert_ids, gate_nums, w_gate, w_up, w_down):
    anywhere = pl.BlockSpec(memory_space=pl.ANY)
    return pl.pallas_call(
        kernel,
        name="routed_experts",
        out_shape=pltpu.VMEM((TOK, D), BF),
        in_specs=[anywhere] * 6,
        out_specs=pl.BlockSpec(memory_space=pltpu.VMEM),
        scratch_shapes=[
            pltpu.VMEM((2, D, FF), BF),
            pltpu.VMEM((2, D, FF), BF),
            pltpu.VMEM((2, FF, D), BF),
            pltpu.VMEM((4, 4, 2, HALF, D), BF),
            pltpu.VMEM((2, 4, 4, 16, TOK), jnp.int32),
            pltpu.VMEM((4, 2, 4, 2, CAP, D), BF),
            pltpu.VMEM((4, 4, 2, CAP, D), BF),
            pltpu.VMEM((4, 4, 2, CAP, D), BF),
            pltpu.VMEM((4, 4, TOK, TOK), BF),
            pltpu.VMEM((4, 2, 2, 4, CAP, TOK), F32),
            pltpu.VMEM((256, FF), BF),
            pltpu.VMEM((4, 2, HALF, D), BF),
            pltpu.VMEM((2, 4, 2, HALF, D), BF),
            pltpu.VMEM((2, HALF, D), BF),
            pltpu.VMEM((2, 2, HALF, D), BF),
            pltpu.VMEM((TOK, TOK), BF),
            pltpu.SemaphoreType.DMA((COPIES,)),
            pltpu.SemaphoreType.DMA((COPIES,)),
            pltpu.SemaphoreType.DMA((3,)),
            pltpu.SemaphoreType.DMA((3, 2)),
        ],
        compiler_params=pltpu.CompilerParams(
            collective_id=0, has_side_effects=True, vmem_limit_bytes=62 * 1024 * 1024
        ),
    )(tokens.reshape(2, HALF, D), expert_ids.T, gate_nums.T, w_gate, w_up, w_down)


def solution(mesh):
    placed = (
        P(("dp", "ep"), None),
        P(("dp", "ep"), None),
        P(("dp", "ep"), None),
        P("ep", None, None),
        P("ep", None, None),
        P("ep", None, None),
    )
    return jax.shard_map(
        shards, mesh=mesh, in_specs=placed, out_specs=P(("dp", "ep"), None), check_vma=False
    )
```

```python
import jax
import jax.numpy as jnp
from jax import lax
from jax.experimental import pallas as pl
from jax.experimental.pallas import tpu as pltpu
from jax.sharding import PartitionSpec as P

MESH = pl.DeviceIdType.MESH
BF = jnp.bfloat16
F32 = jnp.float32
D = 2048
FF = 768
TOK = 128
HALF = 64
CAP = 32
ORDER = (0, 3, 1, 2)
BACK = (2, 3, 1, 0)


def neighbours():
    dp, ep = lax.axis_index("dp"), lax.axis_index("ep")
    z_hi, core = dp // 2, dp % 2
    x, z_lo, y = ep // 8, (ep // 4) % 2, ep % 4
    z = z_hi * 2 + z_lo
    a = (1 - core) * x + core * y
    b = (1 - core) * y + core * x

    def device(a, b, z):
        px = (1 - core) * a + core * b
        py = (1 - core) * b + core * a
        return ((z // 2) * 2 + core, (px * 2 + z % 2) * 4 + py)

    up = z + 1 - 2 * (z % 2)
    down = (z + 3 + 2 * (z % 2)) % 4
    zp = (1 - core) * up + core * down
    where = {
        "a+": device((a + 1) % 4, b, z),
        "a-": device((a + 3) % 4, b, z),
        "a2": device((a + 2) % 4, b, z),
        "b2": device(a, (b + 2) % 4, z),
        "b+": device(a, (b + 1) % 4, z),
        "b-": device(a, (b + 3) % 4, z),
        "z": device(a, b, zp),
    }
    return where, ep, where["z"][1]


def kernel(
    tokens, ids_in, nums_in, wg_in, wu_in, wd_in, out,
    wg, wu, wd, T, M, X, ZS, YR, PS, G, H, FAR, ADJ, FFR, FA, TRI,
    send, recv, local, wsem,
):
    where, ep, pep = neighbours()
    leaving, landing = {}, {}

    def remote(src, dst, to, group, key):
        return pltpu.make_async_remote_copy(
            src_ref=src,
            dst_ref=dst,
            send_sem=send.at[leaving.setdefault(group, len(leaving))],
            recv_sem=recv.at[landing.setdefault(key, len(landing))],
            device_id=where[to],
            device_id_type=MESH,
        )

    def sent(group, ref):
        pltpu.make_async_copy(ref, ref, send.at[leaving[group]]).wait()

    def landed(key, ref):
        pltpu.make_async_copy(ref, ref, recv.at[landing[key]]).wait()

    loads = [
        pltpu.make_async_copy(src, dst, wsem.at[k])
        for k, (src, dst) in enumerate(((wg_in, wg), (wu_in, wu), (wd_in, wd)))
    ]
    own = pltpu.make_async_copy(tokens, T.at[0, 0], local.at[0])
    tables = [
        pltpu.make_async_copy(ids_in, M.at[0, 0, 0, pl.ds(0, 8)], local.at[1]),
        pltpu.make_async_copy(nums_in, M.at[0, 0, 0, pl.ds(8, 8)], local.at[2]),
    ]
    own.start()
    for table in tables:
        table.start()

    mf = [
        remote(M.at[0, 0, 0], M.at[0, 0, 3], "a+", "mf", "mf"),
        remote(M.at[0, 0, 0], M.at[0, 0, 1], "a-", "mf", "mf"),
        remote(M.at[0, 0, 0], M.at[0, 0, 2], "a2", "mf", "mf"),
    ]
    ms = {
        3: remote(M.at[0, 0], M.at[0, 3], "b+", "ms", "ms"),
        1: remote(M.at[0, 0], M.at[0, 1], "b-", "ms", "ms"),
        2: remote(M.at[0, 0], M.at[0, 2], "b2", "ms", "ms"),
    }
    mz = [remote(M.at[0, j], M.at[1, j], "z", "mz", "mz") for j in range(4)]
    f = {}
    for q in range(2):
        part = pl.ds(32 * q, 32)
        f[3, 0, q] = remote(T.at[0, 0, 0, part], T.at[0, 3, 0, part], "a+", "f", ("f", 3, q))
        f[1, 1, q] = remote(T.at[0, 0, 1, part], T.at[0, 1, 1, part], "a+", "f", ("f", 1, q))
        f[2, 0, q] = remote(T.at[0, 3, 0, part], T.at[0, 2, 0, part], "a+", "f", ("f", 2, q))
        f[3, 1, q] = remote(T.at[0, 0, 1, part], T.at[0, 3, 1, part], "a-", "f", ("f", 3, q))
        f[1, 0, q] = remote(T.at[0, 0, 0, part], T.at[0, 1, 0, part], "a-", "f", ("f", 1, q))
        f[2, 1, q] = remote(T.at[0, 3, 1, part], T.at[0, 2, 1, part], "a-", "f", ("f", 2, q))
    s = {}
    for i in range(4):
        s[2, i, 0] = remote(T.at[0, i, 0], T.at[2, i, 0], "b+", "s", ("s", 2, i))
        s[2, i, 1] = remote(T.at[0, i, 1], T.at[2, i, 1], "b-", "s", ("s", 2, i))
        s[1, i, 0] = remote(T.at[2, i, 0], T.at[1, i, 0], "b+", "s", ("s", 1, i))
        s[1, i, 1] = remote(T.at[2, i, 1], T.at[1, i, 1], "b-", "s", ("s", 1, i))
        s[3, i, 1] = remote(T.at[0, i, 1], T.at[3, i, 1], "b+", "s", ("s", 3, i))
        s[3, i, 0] = remote(T.at[0, i, 0], T.at[3, i, 0], "b-", "s", ("s", 3, i))
    zs = {(c, i): remote(ZS.at[c, i], X.at[c, 1, i], "z", "zs", ("zs", c)) for c in range(4) for i in range(4) if c or not i}
    zq = {}
    for i in range(1, 4):
        for q in range(2):
            part = pl.ds(16 * q, 16)
            zq[i, q] = remote(ZS.at[0, i, :, part], X.at[0, 1, i, :, part], "z", "zs", ("zs", 0))
    zr = {(c, i): remote(X.at[c, 1, i], YR.at[c, i], "z", "zr", ("zr", c, i)) for c in range(4) for i in range(4) if (c, i) != (0, 1)}
    zl = []
    for q in range(2):
        part = pl.ds(16 * q, 16)
        zl.append(remote(X.at[0, 1, 1, :, part], YR.at[0, 1, :, part], "z", "zr", ("zl", q)))
    far = {}
    adj = {}
    for i in range(4):
        far[i, 0] = remote(T.at[1, i, 0], FAR.at[i, 0], "b+", "far", ("far", i))
        far[i, 1] = remote(T.at[1, i, 1], FAR.at[i, 1], "b-", "far", ("far", i))
        adj[2, i, 0] = remote(T.at[2, i, 0], ADJ.at[1, i, 0], "b-", "adj", ("adj", i))
        adj[2, i, 1] = remote(T.at[2, i, 1], ADJ.at[0, i, 1], "b+", "adj", ("adj", i))
        adj[3, i, 0] = remote(T.at[3, i, 0], ADJ.at[0, i, 0], "b+", "adj", ("adj", i))
        adj[3, i, 1] = remote(T.at[3, i, 1], ADJ.at[1, i, 1], "b-", "adj", ("adj", i))
    ff = {
        0: remote(T.at[0, 2, 0], FFR.at[0], "a+", "ff", "ff"),
        1: remote(T.at[0, 2, 1], FFR.at[1], "a-", "ff", "ff"),
    }
    fa = {
        (3, 1): remote(T.at[0, 3, 1], FA.at[0, 1], "a+", "fa", "fa"),
        (3, 0): remote(T.at[0, 3, 0], FA.at[1, 0], "a-", "fa", "fa"),
    }
    for q in range(2):
        part = pl.ds(32 * q, 32)
        fa[1, 0, q] = remote(T.at[0, 1, 0, part], FA.at[0, 0, part], "a+", "fa", "fa")
        fa[1, 1, q] = remote(T.at[0, 1, 1, part], FA.at[1, 1, part], "a-", "fa", "fa")

    barrier = pltpu.get_barrier_semaphore()
    peers = ("a+", "a-", "a2", "b+", "b-", "b2", "z")
    for name in peers:
        pl.semaphore_signal(barrier, inc=1, device_id=where[name], device_id_type=MESH)

    lane = lax.broadcasted_iota(jnp.int32, (TOK, TOK), 1)
    row = lax.broadcasted_iota(jnp.int32, (TOK, TOK), 0)
    TRI[...] = jnp.where((row < lane) & ((row & 96) == (lane & 96)), 1.0, 0.0).astype(BF)
    for table in tables:
        table.wait()
    own.wait()
    for load in loads:
        load.start()

    sub8 = lax.broadcasted_iota(jnp.int32, (8, TOK), 0)
    lane8 = lax.broadcasted_iota(jnp.int32, (8, TOK), 1)
    sub32 = lax.broadcasted_iota(jnp.int32, (CAP, TOK), 0).astype(F32)
    expert = jnp.where(sub8 < 2, 2 * ep + sub8, 2 * pep + sub8 - 2)
    start_slot = (((lane8 & 32) >> 1) + ((lane8 & 64) >> 3)).astype(F32)

    low = lax.broadcasted_iota(jnp.int32, (16, TOK), 1) < HALF

    def pick(c, i, plane):
        first, second = ((0, 0), (2, 2), (3, 1), (1, 3))[c]
        return jnp.where(low, M[plane, first, i], M[plane, second, (4 - i) % 4])

    def slots_of(table):
        member = jnp.zeros((8, TOK), F32)
        weight = jnp.zeros((8, TOK), jnp.int32)
        for k in range(8):
            hit = table[k : k + 1] == expert
            member = member + jnp.where(hit, 1.0, 0.0)
            weight = weight + jnp.where(hit, table[8 + k : 9 + k], 0)
        before = jnp.dot(member.astype(BF), TRI[...], preferred_element_type=F32)
        code = jnp.where(member > 0.5, start_slot + before, -1.0)
        return code, weight.astype(F32) * (1.0 / 1024.0)

    def weigh(c, i, plane, hits, gate):
        for e in range(2):
            column = jnp.sum(jnp.where(hits[e], gate[e : e + 1], 0.0), axis=1, keepdims=True)
            G[c, e, plane, i] = jnp.broadcast_to(column, (CAP, TOK))

    def place(c, i):
        code, gate = slots_of(pick(c, i, 0))
        hits = [sub32 == code[r : r + 1] for r in range(4)]
        places = jnp.concatenate([jnp.where(hits[r], 1.0, 0.0) for r in range(4)], axis=0).astype(BF)
        PS[c, i] = places
        weigh(c, i, 0, hits, gate)
        return places

    def pack(c, i):
        places = PS[c, i]
        for n in range(4):
            cols = slice(512 * n, 512 * n + 512)
            rows = T[c, i, :, :, cols].reshape(TOK, 512)
            packed = jnp.dot(places, rows, preferred_element_type=F32).astype(BF)
            X[c, 0, i, :, :, cols] = packed[:HALF].reshape(2, CAP, 512)
            ZS[c, i, :, :, cols] = packed[HALF:].reshape(2, CAP, 512)

    def pack_quarter(i, q):
        part, own = slice(16 * q, 16 * q + 16), slice(32 * q, 32 * q + 32)
        places = jnp.concatenate([PS[0, i, 32 * r + 16 * q : 32 * r + 16 * q + 16] for r in range(4)], axis=0)
        for n in range(4):
            cols = slice(512 * n, 512 * n + 512)
            first, second = T[0, i, 0, own, cols], T[0, i, 1, own, cols]
            rows = jnp.concatenate([first, first, second, second], axis=0)
            packed = jnp.dot(places, rows, preferred_element_type=F32).astype(BF)
            X[0, 0, i, :, part, cols] = packed[:32].reshape(2, 16, 512)
            ZS[0, i, :, part, cols] = packed[32:].reshape(2, 16, 512)
        zq[i, q].start()

    def weigh_theirs(c):
        for i in range(4):
            code, gate = slots_of(pick(c, i, 1))
            weigh(c, i, 1, [sub32 == code[r : r + 1] for r in range(2)], gate)

    def gate_up(c, e, n):
        cols = slice(256 * n, 256 * n + 256) if isinstance(n, int) else pl.ds(pl.multiple_of(n * 256, 256), 256)
        x = X[c, :, :, e].reshape(256, D)
        g = jnp.dot(x, wg[e, :, cols], preferred_element_type=F32)
        u = jnp.dot(x, wu[e, :, cols], preferred_element_type=F32)
        scale = G[c, e].reshape(256, TOK)[:, :1]
        H[:, cols] = (g / (1.0 + jnp.exp(-g)) * u * scale).astype(BF)

    def down(c, e, n):
        cols = pl.ds(pl.multiple_of(n * 512, 512), 512)
        y = jnp.dot(H[...], wd[e, :, cols], preferred_element_type=F32)
        X[c, :, :, e, :, cols] = y.astype(BF).reshape(2, 4, CAP, 512)

    def loop(low, high, step):
        def body(n, carry):
            step(n)
            return carry

        lax.fori_loop(low, high, body, 0)

    def arrived(c):
        landed(("zs", c), X.at[c, 1])
        weigh_theirs(c)

    def fine(c, e):
        return [lambda n=n: gate_up(c, e, n) for n in range(3)] + [
            lambda n=n: loop(n, n + 2, lambda m: down(c, e, m)) for n in (0, 2)
        ]

    def coarse(c, e):
        return [
            lambda: loop(0, 3, lambda n: gate_up(c, e, n)),
            lambda: loop(0, 4, lambda m: down(c, e, m)),
        ]

    def run(steps, count=None):
        for _ in range(len(steps) if count is None else count):
            steps.pop(0)()

    def combine(c, i, extra, target=None):
        for n in range(4):
            cols = slice(512 * n, 512 * n + 512)
            y = jnp.concatenate(
                [X[c, 0, i, :, :, cols].reshape(HALF, 512), YR[c, i, :, :, cols].reshape(HALF, 512)], axis=0
            )
            total = lax.dot_general(PS[c, i], y, (((0,), (0,)), ((), ())), preferred_element_type=F32)
            for part in extra:
                total = total + part[:, :, cols].reshape(TOK, 512).astype(F32)
            if target is None:
                T[c, i, :, :, cols] = total.astype(BF).reshape(2, HALF, 512)
            else:
                target[:, cols] = total.astype(BF)

    def returned(c, i):
        landed(("zr", c, i), YR.at[c, i])
        extra = []
        if c == 3:
            landed(("far", i), FAR.at[i])
            extra = [FAR.at[i]]
        combine(c, i, extra)
        for h in range(2):
            (far[i, h] if c == 1 else adj[c, i, h]).start()

    def pack_send(c, i):
        pack(c, i)
        zs[c, i].start()

    def near(i):
        landed(("s", 2, i), T.at[2, i])
        for h in range(2):
            s[1, i, h].start()
        pack_send(2, i)
        place(1, i)

    def others(i):
        s[3, i, 1].start()
        s[3, i, 0].start()

    def distant(c, i):
        landed(("s", c, i), T.at[c, i])
        pack_send(c, i)
        if c == 1:
            place(3, i)

    place(0, 0)
    pack(0, 0)
    pl.semaphore_wait(barrier, len(peers))
    for q in range(2):
        f[3, 0, q].start()
        f[3, 1, q].start()
        if q == 0:
            for copy in mf:
                copy.start()
            zs[0, 0].start()
    for q in range(2):
        f[1, 1, q].start()
        f[1, 0, q].start()
    for q in range(2):
        landed(("f", 3, q), T.at[0, 3, :, pl.ds(32 * q, 32)])
        for h in range(2):
            f[2, h, q].start()
        if q == 0:
            landed("mf", M.at[0, 0, pl.ds(1, 3)])
            place(0, 3)
            for j in (1, 3, 2):
                ms[j].start()
        pack_quarter(3, q)
    place(0, 1)
    for q in range(2):
        landed(("f", 1, q), T.at[0, 1, :, pl.ds(32 * q, 32)])
        for i in ((), (0, 3, 1))[q]:
            s[2, i, 0].start()
            s[2, i, 1].start()
        pack_quarter(1, q)
    mz[0].start()
    landed("ms", M.at[0, pl.ds(1, 3)])
    for j in (1, 3, 2):
        mz[j].start()
    place(0, 2)
    for i in ORDER:
        place(2, i)
    for q in range(2):
        landed(("f", 2, q), T.at[0, 2, :, pl.ds(32 * q, 32)])
        pack_quarter(2, q)
    s[2, 2, 0].start()
    s[2, 2, 1].start()
    near(0)
    near(3)
    others(0)
    near(1)
    others(3)
    near(2)
    others(1)
    others(2)
    distant(1, 0)
    landed("mz", M.at[1])
    for load in loads:
        load.wait()
    arrived(0)
    first = fine(0, 0)
    run(first, 2)
    distant(1, 3)
    run(first, 2)
    distant(3, 0)
    run(first)
    distant(1, 1)
    arrived(2)
    second = fine(2, 0) + fine(2, 1)
    run(second, 2)
    distant(3, 3)
    run(second, 3)
    distant(1, 2)
    run(second, 2)
    distant(3, 1)
    run(second, 2)
    distant(3, 2)
    run(second)
    for i in BACK:
        zr[2, i].start()
    sent("f", T.at[0, pl.ds(0, 3)])
    sent("s", T.at[pl.ds(0, 3)])
    arrived(1)
    run(coarse(1, 0) + coarse(1, 1))
    arrived(3)
    for i in BACK:
        zr[1, i].start()
    returned(2, 2)
    third = coarse(3, 0) + coarse(3, 1)
    run(third, 1)
    returned(2, 3)
    run(third, 1)
    returned(2, 1)
    run(third, 1)
    returned(2, 0)
    run(third)
    zr[3, 2].start()
    zr[3, 3].start()
    returned(1, 2)
    last = coarse(0, 1)
    run(last, 1)
    returned(1, 3)
    run(last)
    returned(1, 1)
    returned(1, 0)
    zr[0, 2].start()
    zr[3, 1].start()

    def finish(i, extra, target=None):
        landed(("zr", 0, i), YR.at[0, i])
        landed(("adj", i), ADJ.at[:, i])
        combine(0, i, [ADJ.at[0, i], ADJ.at[1, i]] + extra, target)

    returned(3, 2)
    zr[0, 3].start()
    returned(3, 3)
    zr[3, 0].start()
    finish(2, [])
    ff[0].start()
    ff[1].start()
    zl[0].start()
    zl[1].start()
    returned(3, 1)
    zr[0, 0].start()
    finish(3, [])
    fa[3, 0].start()
    fa[3, 1].start()
    returned(3, 0)
    landed(("adj", 1), ADJ.at[:, 1])
    landed("ff", FFR)
    for q in range(2):
        landed(("zl", q), YR.at[0, 1, :, pl.ds(16 * q, 16)])
        part, own = slice(16 * q, 16 * q + 16), slice(32 * q, 32 * q + 32)
        places = jnp.concatenate([PS[0, 1, 32 * r + 16 * q : 32 * r + 16 * q + 16] for r in range(4)], axis=0)
        for n in range(4):
            cols = slice(512 * n, 512 * n + 512)
            y = jnp.concatenate(
                [X[0, 0, 1, :, part, cols].reshape(32, 512), YR[0, 1, :, part, cols].reshape(32, 512)], axis=0
            )
            total = lax.dot_general(places, y, (((0,), (0,)), ((), ())), preferred_element_type=F32)
            for h in range(2):
                rows = total[64 * h + 32 * q : 64 * h + 32 * q + 32]
                for ref in (ADJ.at[0, 1, h], ADJ.at[1, 1, h], FFR.at[h]):
                    rows = rows + ref[own, cols].astype(F32)
                T[0, 1, h, own, cols] = rows.astype(BF)
        fa[1, 0, q].start()
        fa[1, 1, q].start()
    landed("fa", FA)
    finish(0, [FA.at[0], FA.at[1]], out)

    for group, ref in (
        ("mf", M.at[0, 0, pl.ds(0, 3)]), ("ms", M.at[0, pl.ds(0, 3)]), ("mz", M.at[0]), ("zs", ZS), ("zr", YR),
        ("far", FAR), ("adj", ADJ), ("ff", FFR), ("fa", FA),
    ):
        sent(group, ref)


GROUPS = 11
KEYS = 3 + 6 + 12 + 4 + 17 + 4 + 4 + 2


def shards(tokens, expert_ids, gate_nums, w_gate, w_up, w_down):
    anywhere = pl.BlockSpec(memory_space=pl.ANY)
    return pl.pallas_call(
        kernel,
        name="routed_experts",
        out_shape=pltpu.VMEM((TOK, D), BF),
        in_specs=[anywhere] * 6,
        out_specs=pl.BlockSpec(memory_space=pltpu.VMEM),
        scratch_shapes=[
            pltpu.VMEM((2, D, FF), BF),
            pltpu.VMEM((2, D, FF), BF),
            pltpu.VMEM((2, FF, D), BF),
            pltpu.VMEM((4, 4, 2, HALF, D), BF),
            pltpu.VMEM((2, 4, 4, 16, TOK), jnp.int32),
            pltpu.VMEM((4, 2, 4, 2, CAP, D), BF),
            pltpu.VMEM((4, 4, 2, CAP, D), BF),
            pltpu.VMEM((4, 4, 2, CAP, D), BF),
            pltpu.VMEM((4, 4, TOK, TOK), BF),
            pltpu.VMEM((4, 2, 2, 4, CAP, TOK), F32),
            pltpu.VMEM((256, FF), BF),
            pltpu.VMEM((4, 2, HALF, D), BF),
            pltpu.VMEM((2, 4, 2, HALF, D), BF),
            pltpu.VMEM((2, HALF, D), BF),
            pltpu.VMEM((2, 2, HALF, D), BF),
            pltpu.VMEM((TOK, TOK), BF),
            pltpu.SemaphoreType.DMA((GROUPS,)),
            pltpu.SemaphoreType.DMA((KEYS,)),
            pltpu.SemaphoreType.DMA((3,)),
            pltpu.SemaphoreType.DMA((3,)),
        ],
        compiler_params=pltpu.CompilerParams(
            collective_id=0, has_side_effects=True, vmem_limit_bytes=62 * 1024 * 1024
        ),
    )(tokens.reshape(2, HALF, D), expert_ids.T, gate_nums.T, w_gate, w_up, w_down)


def solution(mesh):
    placed = (
        P(("dp", "ep"), None),
        P(("dp", "ep"), None),
        P(("dp", "ep"), None),
        P("ep", None, None),
        P("ep", None, None),
        P("ep", None, None),
    )
    return jax.shard_map(
        shards, mesh=mesh, in_specs=placed, out_specs=P(("dp", "ep"), None), check_vma=False
    )
```

```python
import jax
import jax.numpy as jnp
from jax import lax
from jax.experimental import pallas as pl
from jax.experimental.pallas import tpu as pltpu
from jax.sharding import PartitionSpec as P

MESH = pl.DeviceIdType.MESH
BF = jnp.bfloat16
F32 = jnp.float32
D = 2048
FF = 768
TOK = 128
HALF = 64
CAP = 32
ORDER = (0, 3, 1, 2)
BACK = (2, 3, 1, 0)


def neighbours():
    dp, ep = lax.axis_index("dp"), lax.axis_index("ep")
    z_hi, core = dp // 2, dp % 2
    x, z_lo, y = ep // 8, (ep // 4) % 2, ep % 4
    z = z_hi * 2 + z_lo
    a = (1 - core) * x + core * y
    b = (1 - core) * y + core * x

    def device(a, b, z):
        px = (1 - core) * a + core * b
        py = (1 - core) * b + core * a
        return ((z // 2) * 2 + core, (px * 2 + z % 2) * 4 + py)

    up = z + 1 - 2 * (z % 2)
    down = (z + 3 + 2 * (z % 2)) % 4
    zp = (1 - core) * up + core * down
    where = {
        "a+": device((a + 1) % 4, b, z),
        "a-": device((a + 3) % 4, b, z),
        "a2": device((a + 2) % 4, b, z),
        "b2": device(a, (b + 2) % 4, z),
        "b+": device(a, (b + 1) % 4, z),
        "b-": device(a, (b + 3) % 4, z),
        "z": device(a, b, zp),
    }
    return where, ep, where["z"][1]


def kernel(
    tokens, ids_in, nums_in, wg_in, wu_in, wd_in, out,
    wg, wu, wd, T, M, X, ZS, YR, PS, G, H, FAR, ADJ, FFR, FA, TRI,
    send, recv, local, wsem,
):
    where, ep, pep = neighbours()
    leaving, landing = {}, {}

    def remote(src, dst, to, group, key):
        return pltpu.make_async_remote_copy(
            src_ref=src,
            dst_ref=dst,
            send_sem=send.at[leaving.setdefault(group, len(leaving))],
            recv_sem=recv.at[landing.setdefault(key, len(landing))],
            device_id=where[to],
            device_id_type=MESH,
        )

    def sent(group, ref):
        pltpu.make_async_copy(ref, ref, send.at[leaving[group]]).wait()

    def landed(key, ref):
        pltpu.make_async_copy(ref, ref, recv.at[landing[key]]).wait()

    loads = [
        pltpu.make_async_copy(src, dst, wsem.at[k])
        for k, (src, dst) in enumerate(((wg_in, wg), (wu_in, wu), (wd_in, wd)))
    ]
    own = pltpu.make_async_copy(tokens, T.at[0, 0], local.at[0])
    tables = [
        pltpu.make_async_copy(ids_in, M.at[0, 0, 0, pl.ds(0, 8)], local.at[1]),
        pltpu.make_async_copy(nums_in, M.at[0, 0, 0, pl.ds(8, 8)], local.at[2]),
    ]
    own.start()
    for table in tables:
        table.start()

    mf = [
        remote(M.at[0, 0, 0], M.at[0, 0, 3], "a+", "mf", "mf"),
        remote(M.at[0, 0, 0], M.at[0, 0, 1], "a-", "mf", "mf"),
        remote(M.at[0, 0, 0], M.at[0, 0, 2], "a2", "mf", "mf"),
    ]
    ms = {
        3: remote(M.at[0, 0], M.at[0, 3], "b+", "ms", "ms"),
        1: remote(M.at[0, 0], M.at[0, 1], "b-", "ms", "ms"),
        2: remote(M.at[0, 0], M.at[0, 2], "b2", "ms", "ms"),
    }
    mz = [remote(M.at[0, j], M.at[1, j], "z", "mz", "mz") for j in range(4)]
    f = {}
    for q in range(2):
        part = pl.ds(32 * q, 32)
        f[3, 0, q] = remote(T.at[0, 0, 0, part], T.at[0, 3, 0, part], "a+", "f", ("f", 3, q))
        f[1, 1, q] = remote(T.at[0, 0, 1, part], T.at[0, 1, 1, part], "a+", "f", ("f", 1, q))
        f[2, 0, q] = remote(T.at[0, 3, 0, part], T.at[0, 2, 0, part], "a+", "f", ("f", 2, q))
        f[3, 1, q] = remote(T.at[0, 0, 1, part], T.at[0, 3, 1, part], "a-", "f", ("f", 3, q))
        f[1, 0, q] = remote(T.at[0, 0, 0, part], T.at[0, 1, 0, part], "a-", "f", ("f", 1, q))
        f[2, 1, q] = remote(T.at[0, 3, 1, part], T.at[0, 2, 1, part], "a-", "f", ("f", 2, q))
    s = {}
    for i in range(4):
        s[2, i, 0] = remote(T.at[0, i, 0], T.at[2, i, 0], "b+", "s", ("s", 2, i))
        s[2, i, 1] = remote(T.at[0, i, 1], T.at[2, i, 1], "b-", "s", ("s", 2, i))
        s[1, i, 0] = remote(T.at[2, i, 0], T.at[1, i, 0], "b+", "s", ("s", 1, i))
        s[1, i, 1] = remote(T.at[2, i, 1], T.at[1, i, 1], "b-", "s", ("s", 1, i))
        s[3, i, 1] = remote(T.at[0, i, 1], T.at[3, i, 1], "b+", "s", ("s", 3, i))
        s[3, i, 0] = remote(T.at[0, i, 0], T.at[3, i, 0], "b-", "s", ("s", 3, i))
    zs = {(c, i): remote(ZS.at[c, i], X.at[c, 1, i], "z", "zs", ("zs", c)) for c in range(4) for i in range(4) if c or not i}
    zq = {}
    for i in range(1, 4):
        for q in range(2):
            part = pl.ds(16 * q, 16)
            zq[i, q] = remote(ZS.at[0, i, :, part], X.at[0, 1, i, :, part], "z", "zs", ("zs", 0))
    zr = {(c, i): remote(X.at[c, 1, i], YR.at[c, i], "z", "zr", ("zr", c, i)) for c in range(4) for i in range(4) if (c, i) != (0, 1)}
    zl = []
    for q in range(2):
        part = pl.ds(16 * q, 16)
        zl.append(remote(X.at[0, 1, 1, :, part], YR.at[0, 1, :, part], "z", "zr", ("zl", q)))
    far = {}
    adj = {}
    for i in range(4):
        far[i, 0] = remote(T.at[1, i, 0], FAR.at[i, 0], "b+", "far", ("far", i))
        far[i, 1] = remote(T.at[1, i, 1], FAR.at[i, 1], "b-", "far", ("far", i))
        adj[2, i, 0] = remote(T.at[2, i, 0], ADJ.at[1, i, 0], "b-", "adj", ("adj", i))
        adj[2, i, 1] = remote(T.at[2, i, 1], ADJ.at[0, i, 1], "b+", "adj", ("adj", i))
        adj[3, i, 0] = remote(T.at[3, i, 0], ADJ.at[0, i, 0], "b+", "adj", ("adj", i))
        adj[3, i, 1] = remote(T.at[3, i, 1], ADJ.at[1, i, 1], "b-", "adj", ("adj", i))
    ff = {
        0: remote(T.at[0, 2, 0], FFR.at[0], "a+", "ff", "ff"),
        1: remote(T.at[0, 2, 1], FFR.at[1], "a-", "ff", "ff"),
    }
    fa = {
        (3, 1): remote(T.at[0, 3, 1], FA.at[0, 1], "a+", "fa", "fa"),
        (3, 0): remote(T.at[0, 3, 0], FA.at[1, 0], "a-", "fa", "fa"),
    }
    for q in range(2):
        part = pl.ds(32 * q, 32)
        fa[1, 0, q] = remote(T.at[0, 1, 0, part], FA.at[0, 0, part], "a+", "fa", "fa")
        fa[1, 1, q] = remote(T.at[0, 1, 1, part], FA.at[1, 1, part], "a-", "fa", "fa")

    barrier = pltpu.get_barrier_semaphore()
    peers = ("a+", "a-", "a2", "b+", "b-", "b2", "z")
    for name in peers:
        pl.semaphore_signal(barrier, inc=1, device_id=where[name], device_id_type=MESH)

    lane = lax.broadcasted_iota(jnp.int32, (TOK, TOK), 1)
    row = lax.broadcasted_iota(jnp.int32, (TOK, TOK), 0)
    TRI[...] = jnp.where((row < lane) & ((row & 96) == (lane & 96)), 1.0, 0.0).astype(BF)
    for table in tables:
        table.wait()
    own.wait()
    for load in loads:
        load.start()

    sub8 = lax.broadcasted_iota(jnp.int32, (8, TOK), 0)
    lane8 = lax.broadcasted_iota(jnp.int32, (8, TOK), 1)
    sub32 = lax.broadcasted_iota(jnp.int32, (CAP, TOK), 0).astype(F32)
    expert = jnp.where(sub8 < 2, 2 * ep + sub8, 2 * pep + sub8 - 2)
    start_slot = (((lane8 & 32) >> 1) + ((lane8 & 64) >> 3)).astype(F32)

    low = lax.broadcasted_iota(jnp.int32, (16, TOK), 1) < HALF

    def pick(c, i, plane):
        first, second = ((0, 0), (2, 2), (3, 1), (1, 3))[c]
        return jnp.where(low, M[plane, first, i], M[plane, second, (4 - i) % 4])

    def slots_of(table):
        member = jnp.zeros((8, TOK), F32)
        weight = jnp.zeros((8, TOK), jnp.int32)
        for k in range(8):
            hit = table[k : k + 1] == expert
            member = member + jnp.where(hit, 1.0, 0.0)
            weight = weight + jnp.where(hit, table[8 + k : 9 + k], 0)
        before = jnp.dot(member.astype(BF), TRI[...], preferred_element_type=F32)
        code = jnp.where(member > 0.5, start_slot + before, -1.0)
        return code, weight.astype(F32) * (1.0 / 1024.0)

    def weigh(c, i, plane, hits, gate):
        for e in range(2):
            column = jnp.sum(jnp.where(hits[e], gate[e : e + 1], 0.0), axis=1, keepdims=True)
            G[c, e, plane, i] = jnp.broadcast_to(column, (CAP, TOK))

    def place(c, i):
        code, gate = slots_of(pick(c, i, 0))
        hits = [sub32 == code[r : r + 1] for r in range(4)]
        places = jnp.concatenate([jnp.where(hits[r], 1.0, 0.0) for r in range(4)], axis=0).astype(BF)
        PS[c, i] = places
        weigh(c, i, 0, hits, gate)
        return places

    def pack(c, i):
        places = PS[c, i]
        for n in range(4):
            cols = slice(512 * n, 512 * n + 512)
            rows = T[c, i, :, :, cols].reshape(TOK, 512)
            packed = jnp.dot(places, rows, preferred_element_type=F32).astype(BF)
            X[c, 0, i, :, :, cols] = packed[:HALF].reshape(2, CAP, 512)
            ZS[c, i, :, :, cols] = packed[HALF:].reshape(2, CAP, 512)

    def pack_quarter(i, q):
        part, own = slice(16 * q, 16 * q + 16), slice(32 * q, 32 * q + 32)
        places = jnp.concatenate([PS[0, i, 32 * r + 16 * q : 32 * r + 16 * q + 16] for r in range(4)], axis=0)
        for n in range(4):
            cols = slice(512 * n, 512 * n + 512)
            first, second = T[0, i, 0, own, cols], T[0, i, 1, own, cols]
            rows = jnp.concatenate([first, first, second, second], axis=0)
            packed = jnp.dot(places, rows, preferred_element_type=F32).astype(BF)
            X[0, 0, i, :, part, cols] = packed[:32].reshape(2, 16, 512)
            ZS[0, i, :, part, cols] = packed[32:].reshape(2, 16, 512)
        zq[i, q].start()

    def weigh_theirs(c):
        for i in range(4):
            code, gate = slots_of(pick(c, i, 1))
            weigh(c, i, 1, [sub32 == code[r : r + 1] for r in range(2)], gate)

    def gate_up(c, e, n):
        cols = slice(256 * n, 256 * n + 256) if isinstance(n, int) else pl.ds(pl.multiple_of(n * 256, 256), 256)
        x = X[c, :, :, e].reshape(256, D)
        g = jnp.dot(x, wg[e, :, cols], preferred_element_type=F32)
        u = jnp.dot(x, wu[e, :, cols], preferred_element_type=F32)
        scale = G[c, e].reshape(256, TOK)[:, :1]
        H[:, cols] = (g / (1.0 + jnp.exp(-g)) * u * scale).astype(BF)

    def down(c, e, n):
        cols = pl.ds(pl.multiple_of(n * 512, 512), 512)
        y = jnp.dot(H[...], wd[e, :, cols], preferred_element_type=F32)
        X[c, :, :, e, :, cols] = y.astype(BF).reshape(2, 4, CAP, 512)

    def loop(low, high, step):
        def body(n, carry):
            step(n)
            return carry

        lax.fori_loop(low, high, body, 0)

    def arrived(c):
        landed(("zs", c), X.at[c, 1])
        weigh_theirs(c)

    def fine(c, e):
        return [lambda n=n: gate_up(c, e, n) for n in range(3)] + [
            lambda n=n: loop(n, n + 2, lambda m: down(c, e, m)) for n in (0, 2)
        ]

    def coarse(c, e):
        return [
            lambda: loop(0, 3, lambda n: gate_up(c, e, n)),
            lambda: loop(0, 4, lambda m: down(c, e, m)),
        ]

    def run(steps, count=None):
        for _ in range(len(steps) if count is None else count):
            steps.pop(0)()

    def combine(c, i, extra, target=None):
        for n in range(4):
            cols = slice(512 * n, 512 * n + 512)
            y = jnp.concatenate(
                [X[c, 0, i, :, :, cols].reshape(HALF, 512), YR[c, i, :, :, cols].reshape(HALF, 512)], axis=0
            )
            total = lax.dot_general(PS[c, i], y, (((0,), (0,)), ((), ())), preferred_element_type=F32)
            for part in extra:
                total = total + part[:, :, cols].reshape(TOK, 512).astype(F32)
            if target is None:
                T[c, i, :, :, cols] = total.astype(BF).reshape(2, HALF, 512)
            else:
                target[:, cols] = total.astype(BF)

    def returned(c, i):
        landed(("zr", c, i), YR.at[c, i])
        extra = []
        if c == 3:
            landed(("far", i), FAR.at[i])
            extra = [FAR.at[i]]
        combine(c, i, extra)
        for h in range(2):
            (far[i, h] if c == 1 else adj[c, i, h]).start()

    def pack_send(c, i):
        pack(c, i)
        zs[c, i].start()

    def near(i):
        landed(("s", 2, i), T.at[2, i])
        for h in range(2):
            s[1, i, h].start()
        pack_send(2, i)
        place(1, i)

    def others(i):
        s[3, i, 1].start()
        s[3, i, 0].start()

    def distant(c, i):
        landed(("s", c, i), T.at[c, i])
        pack_send(c, i)
        if c == 1:
            place(3, i)

    place(0, 0)
    pack(0, 0)
    pl.semaphore_wait(barrier, len(peers))
    for q in range(2):
        f[3, 0, q].start()
        f[3, 1, q].start()
        if q == 0:
            for copy in mf:
                copy.start()
            zs[0, 0].start()
    for q in range(2):
        f[1, 1, q].start()
        f[1, 0, q].start()
    for q in range(2):
        landed(("f", 3, q), T.at[0, 3, :, pl.ds(32 * q, 32)])
        for h in range(2):
            f[2, h, q].start()
        if q == 0:
            landed("mf", M.at[0, 0, pl.ds(1, 3)])
            place(0, 3)
            for j in (1, 3, 2):
                ms[j].start()
        pack_quarter(3, q)
    place(0, 1)
    for q in range(2):
        landed(("f", 1, q), T.at[0, 1, :, pl.ds(32 * q, 32)])
        for i in ((), (0, 3, 1))[q]:
            s[2, i, 0].start()
            s[2, i, 1].start()
        pack_quarter(1, q)
    mz[0].start()
    landed("ms", M.at[0, pl.ds(1, 3)])
    for j in (1, 3, 2):
        mz[j].start()
    place(0, 2)
    for i in ORDER:
        place(2, i)
    for q in range(2):
        landed(("f", 2, q), T.at[0, 2, :, pl.ds(32 * q, 32)])
        pack_quarter(2, q)
    s[2, 2, 0].start()
    s[2, 2, 1].start()
    near(0)
    near(3)
    others(0)
    near(1)
    others(3)
    near(2)
    others(1)
    others(2)
    distant(1, 0)
    landed("mz", M.at[1])
    for load in loads:
        load.wait()
    arrived(0)
    first = fine(0, 0)
    run(first, 2)
    distant(1, 3)
    run(first, 2)
    distant(3, 0)
    run(first)
    distant(1, 1)
    arrived(2)
    second = fine(2, 0) + fine(2, 1)
    run(second, 2)
    distant(3, 3)
    run(second, 3)
    distant(1, 2)
    run(second, 2)
    distant(3, 1)
    run(second, 2)
    distant(3, 2)
    run(second)
    for i in BACK:
        zr[2, i].start()
    sent("f", T.at[0, pl.ds(0, 3)])
    sent("s", T.at[pl.ds(0, 3)])
    arrived(1)
    run(coarse(1, 0) + coarse(1, 1))
    arrived(3)
    for i in BACK:
        zr[1, i].start()
    returned(2, 2)
    third = coarse(3, 0) + coarse(3, 1)
    run(third, 1)
    returned(2, 3)
    run(third, 1)
    returned(2, 1)
    run(third, 1)
    returned(2, 0)
    run(third)
    zr[3, 2].start()
    zr[3, 3].start()
    returned(1, 2)
    last = coarse(0, 1)
    run(last, 1)
    returned(1, 3)
    run(last)
    returned(1, 1)
    returned(1, 0)
    zr[3, 1].start()
    zr[0, 2].start()

    def finish(i, extra, target=None):
        landed(("zr", 0, i), YR.at[0, i])
        landed(("adj", i), ADJ.at[:, i])
        combine(0, i, [ADJ.at[0, i], ADJ.at[1, i]] + extra, target)

    returned(3, 2)
    zr[3, 0].start()
    returned(3, 3)
    zr[0, 3].start()
    returned(3, 1)
    zl[0].start()
    zl[1].start()
    finish(2, [])
    ff[0].start()
    ff[1].start()
    zr[0, 0].start()
    returned(3, 0)
    finish(3, [])
    fa[3, 0].start()
    fa[3, 1].start()
    landed(("adj", 1), ADJ.at[:, 1])
    landed("ff", FFR)
    for q in range(2):
        landed(("zl", q), YR.at[0, 1, :, pl.ds(16 * q, 16)])
        part, own = slice(16 * q, 16 * q + 16), slice(32 * q, 32 * q + 32)
        places = jnp.concatenate([PS[0, 1, 32 * r + 16 * q : 32 * r + 16 * q + 16] for r in range(4)], axis=0)
        for n in range(4):
            cols = slice(512 * n, 512 * n + 512)
            y = jnp.concatenate(
                [X[0, 0, 1, :, part, cols].reshape(32, 512), YR[0, 1, :, part, cols].reshape(32, 512)], axis=0
            )
            total = lax.dot_general(places, y, (((0,), (0,)), ((), ())), preferred_element_type=F32)
            for h in range(2):
                rows = total[64 * h + 32 * q : 64 * h + 32 * q + 32]
                for ref in (ADJ.at[0, 1, h], ADJ.at[1, 1, h], FFR.at[h]):
                    rows = rows + ref[own, cols].astype(F32)
                T[0, 1, h, own, cols] = rows.astype(BF)
        fa[1, 0, q].start()
        fa[1, 1, q].start()
    landed("fa", FA)
    finish(0, [FA.at[0], FA.at[1]], out)

    for group, ref in (
        ("mf", M.at[0, 0, pl.ds(0, 3)]), ("ms", M.at[0, pl.ds(0, 3)]), ("mz", M.at[0]), ("zs", ZS), ("zr", YR),
        ("far", FAR), ("adj", ADJ), ("ff", FFR), ("fa", FA),
    ):
        sent(group, ref)


GROUPS = 11
KEYS = 3 + 6 + 12 + 4 + 17 + 4 + 4 + 2


def shards(tokens, expert_ids, gate_nums, w_gate, w_up, w_down):
    anywhere = pl.BlockSpec(memory_space=pl.ANY)
    return pl.pallas_call(
        kernel,
        name="routed_experts",
        out_shape=pltpu.VMEM((TOK, D), BF),
        in_specs=[anywhere] * 6,
        out_specs=pl.BlockSpec(memory_space=pltpu.VMEM),
        scratch_shapes=[
            pltpu.VMEM((2, D, FF), BF),
            pltpu.VMEM((2, D, FF), BF),
            pltpu.VMEM((2, FF, D), BF),
            pltpu.VMEM((4, 4, 2, HALF, D), BF),
            pltpu.VMEM((2, 4, 4, 16, TOK), jnp.int32),
            pltpu.VMEM((4, 2, 4, 2, CAP, D), BF),
            pltpu.VMEM((4, 4, 2, CAP, D), BF),
            pltpu.VMEM((4, 4, 2, CAP, D), BF),
            pltpu.VMEM((4, 4, TOK, TOK), BF),
            pltpu.VMEM((4, 2, 2, 4, CAP, TOK), F32),
            pltpu.VMEM((256, FF), BF),
            pltpu.VMEM((4, 2, HALF, D), BF),
            pltpu.VMEM((2, 4, 2, HALF, D), BF),
            pltpu.VMEM((2, HALF, D), BF),
            pltpu.VMEM((2, 2, HALF, D), BF),
            pltpu.VMEM((TOK, TOK), BF),
            pltpu.SemaphoreType.DMA((GROUPS,)),
            pltpu.SemaphoreType.DMA((KEYS,)),
            pltpu.SemaphoreType.DMA((3,)),
            pltpu.SemaphoreType.DMA((3,)),
        ],
        compiler_params=pltpu.CompilerParams(
            collective_id=0, has_side_effects=True, vmem_limit_bytes=62 * 1024 * 1024
        ),
    )(tokens.reshape(2, HALF, D), expert_ids.T, gate_nums.T, w_gate, w_up, w_down)


def solution(mesh):
    placed = (
        P(("dp", "ep"), None),
        P(("dp", "ep"), None),
        P(("dp", "ep"), None),
        P("ep", None, None),
        P("ep", None, None),
        P("ep", None, None),
    )
    return jax.shard_map(
        shards, mesh=mesh, in_specs=placed, out_specs=P(("dp", "ep"), None), check_vma=False
    )
```

```python
import jax
import jax.numpy as jnp
from jax import lax
from jax.experimental import pallas as pl
from jax.experimental.pallas import tpu as pltpu
from jax.sharding import PartitionSpec as P

MESH = pl.DeviceIdType.MESH
BF = jnp.bfloat16
F32 = jnp.float32
D = 2048
FF = 768
TOK = 128
HALF = 64
CAP = 32
ORDER = (0, 3, 1, 2)
BACK = (2, 3, 1, 0)


def neighbours():
    dp, ep = lax.axis_index("dp"), lax.axis_index("ep")
    z_hi, core = dp // 2, dp % 2
    x, z_lo, y = ep // 8, (ep // 4) % 2, ep % 4
    z = z_hi * 2 + z_lo
    a = (1 - core) * x + core * y
    b = (1 - core) * y + core * x

    def device(a, b, z):
        px = (1 - core) * a + core * b
        py = (1 - core) * b + core * a
        return ((z // 2) * 2 + core, (px * 2 + z % 2) * 4 + py)

    up = z + 1 - 2 * (z % 2)
    down = (z + 3 + 2 * (z % 2)) % 4
    zp = (1 - core) * up + core * down
    where = {
        "a+": device((a + 1) % 4, b, z),
        "a-": device((a + 3) % 4, b, z),
        "a2": device((a + 2) % 4, b, z),
        "b2": device(a, (b + 2) % 4, z),
        "b+": device(a, (b + 1) % 4, z),
        "b-": device(a, (b + 3) % 4, z),
        "z": device(a, b, zp),
    }
    return where, ep, where["z"][1]


def kernel(
    tokens, ids_in, nums_in, wg_in, wu_in, wd_in, out,
    wg, wu, wd, T, M, X, ZS, YR, PS, G, H, FAR, ADJ, FFR, FA, SUM, TRI,
    send, recv, local, wsem,
):
    where, ep, pep = neighbours()
    leaving, landing = {}, {}

    def remote(src, dst, to, group, key):
        return pltpu.make_async_remote_copy(
            src_ref=src,
            dst_ref=dst,
            send_sem=send.at[leaving.setdefault(group, len(leaving))],
            recv_sem=recv.at[landing.setdefault(key, len(landing))],
            device_id=where[to],
            device_id_type=MESH,
        )

    def sent(group, ref):
        pltpu.make_async_copy(ref, ref, send.at[leaving[group]]).wait()

    def landed(key, ref):
        pltpu.make_async_copy(ref, ref, recv.at[landing[key]]).wait()

    loads = [
        pltpu.make_async_copy(src, dst, wsem.at[k])
        for k, (src, dst) in enumerate(((wg_in, wg), (wu_in, wu), (wd_in, wd)))
    ]
    own = pltpu.make_async_copy(tokens, T.at[0, 0], local.at[0])
    tables = [
        pltpu.make_async_copy(ids_in, M.at[0, 0, 0, pl.ds(0, 8)], local.at[1]),
        pltpu.make_async_copy(nums_in, M.at[0, 0, 0, pl.ds(8, 8)], local.at[2]),
    ]
    own.start()
    for table in tables:
        table.start()

    mf = [
        remote(M.at[0, 0, 0], M.at[0, 0, 3], "a+", "mf", "mf"),
        remote(M.at[0, 0, 0], M.at[0, 0, 1], "a-", "mf", "mf"),
        remote(M.at[0, 0, 0], M.at[0, 0, 2], "a2", "mf", "mf"),
    ]
    ms = {
        3: remote(M.at[0, 0], M.at[0, 3], "b+", "ms", "ms"),
        1: remote(M.at[0, 0], M.at[0, 1], "b-", "ms", "ms"),
        2: remote(M.at[0, 0], M.at[0, 2], "b2", "ms", "ms"),
    }
    mz = [remote(M.at[0, j], M.at[1, j], "z", "mz", "mz") for j in range(4)]
    f = {}
    for q in range(2):
        part = pl.ds(32 * q, 32)
        f[3, 0, q] = remote(T.at[0, 0, 0, part], T.at[0, 3, 0, part], "a+", "f", ("f", 3, q))
        f[1, 1, q] = remote(T.at[0, 0, 1, part], T.at[0, 1, 1, part], "a+", "f", ("f", 1, q))
        f[2, 0, q] = remote(T.at[0, 3, 0, part], T.at[0, 2, 0, part], "a+", "f", ("f", 2, q))
        f[3, 1, q] = remote(T.at[0, 0, 1, part], T.at[0, 3, 1, part], "a-", "f", ("f", 3, q))
        f[1, 0, q] = remote(T.at[0, 0, 0, part], T.at[0, 1, 0, part], "a-", "f", ("f", 1, q))
        f[2, 1, q] = remote(T.at[0, 3, 1, part], T.at[0, 2, 1, part], "a-", "f", ("f", 2, q))
    s = {}
    for i in range(4):
        s[2, i, 0] = remote(T.at[0, i, 0], T.at[2, i, 0], "b+", "s", ("s", 2, i))
        s[2, i, 1] = remote(T.at[0, i, 1], T.at[2, i, 1], "b-", "s", ("s", 2, i))
        s[1, i, 0] = remote(T.at[2, i, 0], T.at[1, i, 0], "b+", "s", ("s", 1, i))
        s[1, i, 1] = remote(T.at[2, i, 1], T.at[1, i, 1], "b-", "s", ("s", 1, i))
        s[3, i, 1] = remote(T.at[0, i, 1], T.at[3, i, 1], "b+", "s", ("s", 3, i))
        s[3, i, 0] = remote(T.at[0, i, 0], T.at[3, i, 0], "b-", "s", ("s", 3, i))
    zs = {(c, i): remote(ZS.at[c, i], X.at[c, 1, i], "z", "zs", ("zs", c)) for c in range(4) for i in range(4) if c or not i}
    zq = {}
    for i in range(1, 4):
        for q in range(2):
            part = pl.ds(16 * q, 16)
            zq[i, q] = remote(ZS.at[0, i, :, part], X.at[0, 1, i, :, part], "z", "zs", ("zs", 0))
    zr = {(c, i): remote(X.at[c, 1, i], YR.at[c, i], "z", "zr", ("zr", c, i)) for c in range(4) for i in range(4) if (c, i) != (0, 1)}
    zl = []
    for q in range(2):
        part = pl.ds(16 * q, 16)
        zl.append(remote(X.at[0, 1, 1, :, part], YR.at[0, 1, :, part], "z", "zr", ("zl", q)))
    far = {}
    adj = {}
    for i in range(4):
        far[i, 0] = remote(T.at[1, i, 0], FAR.at[i, 0], "b+", "far", ("far", i))
        far[i, 1] = remote(T.at[1, i, 1], FAR.at[i, 1], "b-", "far", ("far", i))
        adj[2, i, 0] = remote(T.at[2, i, 0], ADJ.at[1, i, 0], "b-", "adj", ("adj", i))
        adj[2, i, 1] = remote(T.at[2, i, 1], ADJ.at[0, i, 1], "b+", "adj", ("adj", i))
        adj[3, i, 0] = remote(T.at[3, i, 0], ADJ.at[0, i, 0], "b+", "adj", ("adj", i))
        adj[3, i, 1] = remote(T.at[3, i, 1], ADJ.at[1, i, 1], "b-", "adj", ("adj", i))
    ff = {
        0: remote(T.at[0, 2, 0], FFR.at[0], "a+", "ff", "ff"),
        1: remote(T.at[0, 2, 1], FFR.at[1], "a-", "ff", "ff"),
    }
    fa = {
        (3, 1): remote(T.at[0, 3, 1], FA.at[0, 1], "a+", "fa", "fa"),
        (3, 0): remote(T.at[0, 3, 0], FA.at[1, 0], "a-", "fa", "fa"),
    }
    for q in range(2):
        part = pl.ds(32 * q, 32)
        fa[1, 0, q] = remote(T.at[0, 1, 0, part], FA.at[0, 0, part], "a+", "fa", "fa")
        fa[1, 1, q] = remote(T.at[0, 1, 1, part], FA.at[1, 1, part], "a-", "fa", "fa")

    barrier = pltpu.get_barrier_semaphore()
    peers = ("a+", "a-", "a2", "b+", "b-", "b2", "z")
    for name in peers:
        pl.semaphore_signal(barrier, inc=1, device_id=where[name], device_id_type=MESH)

    lane = lax.broadcasted_iota(jnp.int32, (TOK, TOK), 1)
    row = lax.broadcasted_iota(jnp.int32, (TOK, TOK), 0)
    TRI[...] = jnp.where((row < lane) & ((row & 96) == (lane & 96)), 1.0, 0.0).astype(BF)
    for table in tables:
        table.wait()
    own.wait()
    for load in loads:
        load.start()

    sub8 = lax.broadcasted_iota(jnp.int32, (8, TOK), 0)
    lane8 = lax.broadcasted_iota(jnp.int32, (8, TOK), 1)
    sub32 = lax.broadcasted_iota(jnp.int32, (CAP, TOK), 0).astype(F32)
    expert = jnp.where(sub8 < 2, 2 * ep + sub8, 2 * pep + sub8 - 2)
    start_slot = (((lane8 & 32) >> 1) + ((lane8 & 64) >> 3)).astype(F32)

    low = lax.broadcasted_iota(jnp.int32, (16, TOK), 1) < HALF

    def pick(c, i, plane):
        first, second = ((0, 0), (2, 2), (3, 1), (1, 3))[c]
        return jnp.where(low, M[plane, first, i], M[plane, second, (4 - i) % 4])

    def slots_of(table):
        member = jnp.zeros((8, TOK), F32)
        weight = jnp.zeros((8, TOK), jnp.int32)
        for k in range(8):
            hit = table[k : k + 1] == expert
            member = member + jnp.where(hit, 1.0, 0.0)
            weight = weight + jnp.where(hit, table[8 + k : 9 + k], 0)
        before = jnp.dot(member.astype(BF), TRI[...], preferred_element_type=F32)
        code = jnp.where(member > 0.5, start_slot + before, -1.0)
        return code, weight.astype(F32) * (1.0 / 1024.0)

    def weigh(c, i, plane, hits, gate):
        for e in range(2):
            column = jnp.sum(jnp.where(hits[e], gate[e : e + 1], 0.0), axis=1, keepdims=True)
            G[c, e, plane, i] = jnp.broadcast_to(column, (CAP, TOK))

    def place(c, i):
        code, gate = slots_of(pick(c, i, 0))
        hits = [sub32 == code[r : r + 1] for r in range(4)]
        places = jnp.concatenate([jnp.where(hits[r], 1.0, 0.0) for r in range(4)], axis=0).astype(BF)
        PS[c, i] = places
        weigh(c, i, 0, hits, gate)
        return places

    def pack(c, i):
        places = PS[c, i]
        for n in range(4):
            cols = slice(512 * n, 512 * n + 512)
            rows = T[c, i, :, :, cols].reshape(TOK, 512)
            packed = jnp.dot(places, rows, preferred_element_type=F32).astype(BF)
            X[c, 0, i, :, :, cols] = packed[:HALF].reshape(2, CAP, 512)
            ZS[c, i, :, :, cols] = packed[HALF:].reshape(2, CAP, 512)

    def pack_quarter(i, q):
        part, own = slice(16 * q, 16 * q + 16), slice(32 * q, 32 * q + 32)
        places = jnp.concatenate([PS[0, i, 32 * r + 16 * q : 32 * r + 16 * q + 16] for r in range(4)], axis=0)
        for n in range(4):
            cols = slice(512 * n, 512 * n + 512)
            first, second = T[0, i, 0, own, cols], T[0, i, 1, own, cols]
            rows = jnp.concatenate([first, first, second, second], axis=0)
            packed = jnp.dot(places, rows, preferred_element_type=F32).astype(BF)
            X[0, 0, i, :, part, cols] = packed[:32].reshape(2, 16, 512)
            ZS[0, i, :, part, cols] = packed[32:].reshape(2, 16, 512)
        zq[i, q].start()

    def weigh_theirs(c):
        for i in range(4):
            code, gate = slots_of(pick(c, i, 1))
            weigh(c, i, 1, [sub32 == code[r : r + 1] for r in range(2)], gate)

    def gate_up(c, e, n):
        cols = slice(256 * n, 256 * n + 256) if isinstance(n, int) else pl.ds(pl.multiple_of(n * 256, 256), 256)
        x = X[c, :, :, e].reshape(256, D)
        g = jnp.dot(x, wg[e, :, cols], preferred_element_type=F32)
        u = jnp.dot(x, wu[e, :, cols], preferred_element_type=F32)
        scale = G[c, e].reshape(256, TOK)[:, :1]
        H[:, cols] = (g / (1.0 + jnp.exp(-g)) * u * scale).astype(BF)

    def down(c, e, n):
        cols = pl.ds(pl.multiple_of(n * 512, 512), 512)
        y = jnp.dot(H[...], wd[e, :, cols], preferred_element_type=F32)
        X[c, :, :, e, :, cols] = y.astype(BF).reshape(2, 4, CAP, 512)

    def loop(low, high, step):
        def body(n, carry):
            step(n)
            return carry

        lax.fori_loop(low, high, body, 0)

    def arrived(c):
        landed(("zs", c), X.at[c, 1])
        weigh_theirs(c)

    def fine(c, e):
        return [lambda n=n: gate_up(c, e, n) for n in range(3)] + [
            lambda n=n: loop(n, n + 2, lambda m: down(c, e, m)) for n in (0, 2)
        ]

    def coarse(c, e):
        return [
            lambda: loop(0, 3, lambda n: gate_up(c, e, n)),
            lambda: loop(0, 4, lambda m: down(c, e, m)),
        ]

    def run(steps, count=None):
        for _ in range(len(steps) if count is None else count):
            steps.pop(0)()

    def combine(c, i, extra, target=None):
        for n in range(4):
            cols = slice(512 * n, 512 * n + 512)
            y = jnp.concatenate(
                [X[c, 0, i, :, :, cols].reshape(HALF, 512), YR[c, i, :, :, cols].reshape(HALF, 512)], axis=0
            )
            total = lax.dot_general(PS[c, i], y, (((0,), (0,)), ((), ())), preferred_element_type=F32)
            for part in extra:
                total = total + part[:, :, cols].reshape(TOK, 512).astype(F32)
            if target is None:
                T[c, i, :, :, cols] = total.astype(BF).reshape(2, HALF, 512)
            else:
                target[:, :, cols] = total.reshape(2, HALF, 512)

    def returned(c, i):
        landed(("zr", c, i), YR.at[c, i])
        extra = []
        if c == 3:
            landed(("far", i), FAR.at[i])
            extra = [FAR.at[i]]
        combine(c, i, extra)
        for h in range(2):
            (far[i, h] if c == 1 else adj[c, i, h]).start()

    def pack_send(c, i):
        pack(c, i)
        zs[c, i].start()

    def near(i):
        landed(("s", 2, i), T.at[2, i])
        for h in range(2):
            s[1, i, h].start()
        pack_send(2, i)
        place(1, i)

    def others(i):
        s[3, i, 1].start()
        s[3, i, 0].start()

    def distant(c, i):
        landed(("s", c, i), T.at[c, i])
        pack_send(c, i)
        if c == 1:
            place(3, i)

    place(0, 0)
    pack(0, 0)
    pl.semaphore_wait(barrier, len(peers))
    for q in range(2):
        f[3, 0, q].start()
        f[3, 1, q].start()
        if q == 0:
            for copy in mf:
                copy.start()
            zs[0, 0].start()
    for q in range(2):
        f[1, 1, q].start()
        f[1, 0, q].start()
    for q in range(2):
        landed(("f", 3, q), T.at[0, 3, :, pl.ds(32 * q, 32)])
        for h in range(2):
            f[2, h, q].start()
        if q == 0:
            landed("mf", M.at[0, 0, pl.ds(1, 3)])
            place(0, 3)
            for j in (1, 3, 2):
                ms[j].start()
        pack_quarter(3, q)
    place(0, 1)
    for q in range(2):
        landed(("f", 1, q), T.at[0, 1, :, pl.ds(32 * q, 32)])
        for i in ((), (0, 3, 1))[q]:
            s[2, i, 0].start()
            s[2, i, 1].start()
        pack_quarter(1, q)
    mz[0].start()
    landed("ms", M.at[0, pl.ds(1, 3)])
    for j in (1, 3, 2):
        mz[j].start()
    place(0, 2)
    for i in ORDER:
        place(2, i)
    for q in range(2):
        landed(("f", 2, q), T.at[0, 2, :, pl.ds(32 * q, 32)])
        pack_quarter(2, q)
    s[2, 2, 0].start()
    s[2, 2, 1].start()
    near(0)
    near(3)
    others(0)
    near(1)
    others(3)
    near(2)
    others(1)
    others(2)
    distant(1, 0)
    landed("mz", M.at[1])
    for load in loads:
        load.wait()
    arrived(0)
    first = fine(0, 0)
    run(first, 2)
    distant(1, 3)
    run(first, 2)
    distant(3, 0)
    run(first)
    distant(1, 1)
    arrived(2)
    second = fine(2, 0) + fine(2, 1)
    run(second, 2)
    distant(3, 3)
    run(second, 3)
    distant(1, 2)
    run(second, 2)
    distant(3, 1)
    run(second, 2)
    distant(3, 2)
    run(second)
    for i in BACK:
        zr[2, i].start()
    sent("f", T.at[0, pl.ds(0, 3)])
    sent("s", T.at[pl.ds(0, 3)])
    arrived(1)
    run(coarse(1, 0) + coarse(1, 1))
    arrived(3)
    for i in BACK:
        zr[1, i].start()
    returned(2, 2)
    third = coarse(3, 0) + coarse(3, 1)
    run(third, 1)
    returned(2, 3)
    run(third, 1)
    returned(2, 1)
    run(third, 1)
    returned(2, 0)
    run(third)
    zr[3, 2].start()
    zr[3, 3].start()
    returned(1, 2)
    last = coarse(0, 1)
    run(last, 1)
    returned(1, 3)
    run(last)
    returned(1, 1)
    returned(1, 0)
    zr[3, 1].start()
    zr[0, 2].start()

    def finish(i, extra, target=None):
        landed(("zr", 0, i), YR.at[0, i])
        landed(("adj", i), ADJ.at[:, i])
        combine(0, i, [ADJ.at[0, i], ADJ.at[1, i]] + extra, target)

    returned(3, 2)
    zr[3, 0].start()
    returned(3, 3)
    zr[0, 3].start()
    returned(3, 1)
    zl[0].start()
    zl[1].start()
    finish(2, [])
    ff[0].start()
    ff[1].start()
    zr[0, 0].start()
    returned(3, 0)
    finish(3, [])
    fa[3, 0].start()
    fa[3, 1].start()
    landed(("adj", 1), ADJ.at[:, 1])
    landed("ff", FFR)
    for n in range(4):
        cols = slice(512 * n, 512 * n + 512)
        known = [ref[:, :, cols].astype(F32) for ref in (ADJ.at[0, 1], ADJ.at[1, 1], FFR)]
        SUM[:, :, cols] = known[0] + known[1] + known[2]
    for q in range(2):
        landed(("zl", q), YR.at[0, 1, :, pl.ds(16 * q, 16)])
        part, own = slice(16 * q, 16 * q + 16), slice(32 * q, 32 * q + 32)
        places = jnp.concatenate([PS[0, 1, 32 * r + 16 * q : 32 * r + 16 * q + 16] for r in range(4)], axis=0)
        for n in range(4):
            cols = slice(512 * n, 512 * n + 512)
            y = jnp.concatenate(
                [X[0, 0, 1, :, part, cols].reshape(32, 512), YR[0, 1, :, part, cols].reshape(32, 512)], axis=0
            )
            total = lax.dot_general(places, y, (((0,), (0,)), ((), ())), preferred_element_type=F32)
            for h in range(2):
                rows = total[64 * h + 32 * q : 64 * h + 32 * q + 32]
                T[0, 1, h, own, cols] = (rows + SUM[h, own, cols]).astype(BF)
        fa[1, 0, q].start()
        fa[1, 1, q].start()
    finish(0, [], SUM)
    landed("fa", FA)
    for n in range(4):
        cols = slice(512 * n, 512 * n + 512)
        total = SUM[:, :, cols] + FA[0, :, :, cols].astype(F32) + FA[1, :, :, cols].astype(F32)
        out[:, cols] = total.astype(BF).reshape(TOK, 512)

    for group, ref in (
        ("mf", M.at[0, 0, pl.ds(0, 3)]), ("ms", M.at[0, pl.ds(0, 3)]), ("mz", M.at[0]), ("zs", ZS), ("zr", YR),
        ("far", FAR), ("adj", ADJ), ("ff", FFR), ("fa", FA),
    ):
        sent(group, ref)


GROUPS = 11
KEYS = 3 + 6 + 12 + 4 + 17 + 4 + 4 + 2


def shards(tokens, expert_ids, gate_nums, w_gate, w_up, w_down):
    anywhere = pl.BlockSpec(memory_space=pl.ANY)
    return pl.pallas_call(
        kernel,
        name="routed_experts",
        out_shape=pltpu.VMEM((TOK, D), BF),
        in_specs=[anywhere] * 6,
        out_specs=pl.BlockSpec(memory_space=pltpu.VMEM),
        scratch_shapes=[
            pltpu.VMEM((2, D, FF), BF),
            pltpu.VMEM((2, D, FF), BF),
            pltpu.VMEM((2, FF, D), BF),
            pltpu.VMEM((4, 4, 2, HALF, D), BF),
            pltpu.VMEM((2, 4, 4, 16, TOK), jnp.int32),
            pltpu.VMEM((4, 2, 4, 2, CAP, D), BF),
            pltpu.VMEM((4, 4, 2, CAP, D), BF),
            pltpu.VMEM((4, 4, 2, CAP, D), BF),
            pltpu.VMEM((4, 4, TOK, TOK), BF),
            pltpu.VMEM((4, 2, 2, 4, CAP, TOK), F32),
            pltpu.VMEM((256, FF), BF),
            pltpu.VMEM((4, 2, HALF, D), BF),
            pltpu.VMEM((2, 4, 2, HALF, D), BF),
            pltpu.VMEM((2, HALF, D), BF),
            pltpu.VMEM((2, 2, HALF, D), BF),
            pltpu.VMEM((2, HALF, D), F32),
            pltpu.VMEM((TOK, TOK), BF),
            pltpu.SemaphoreType.DMA((GROUPS,)),
            pltpu.SemaphoreType.DMA((KEYS,)),
            pltpu.SemaphoreType.DMA((3,)),
            pltpu.SemaphoreType.DMA((3,)),
        ],
        compiler_params=pltpu.CompilerParams(
            collective_id=0, has_side_effects=True, vmem_limit_bytes=62 * 1024 * 1024
        ),
    )(tokens.reshape(2, HALF, D), expert_ids.T, gate_nums.T, w_gate, w_up, w_down)


def solution(mesh):
    placed = (
        P(("dp", "ep"), None),
        P(("dp", "ep"), None),
        P(("dp", "ep"), None),
        P("ep", None, None),
        P("ep", None, None),
        P("ep", None, None),
    )
    return jax.shard_map(
        shards, mesh=mesh, in_specs=placed, out_specs=P(("dp", "ep"), None), check_vma=False
    )
```

```python
import jax
import jax.numpy as jnp
from jax import lax
from jax.experimental import pallas as pl
from jax.experimental.pallas import tpu as pltpu
from jax.sharding import PartitionSpec as P

MESH = pl.DeviceIdType.MESH
BF = jnp.bfloat16
F32 = jnp.float32
D = 2048
FF = 768
TOK = 128
HALF = 64
CAP = 32
ORDER = (0, 3, 1, 2)
BACK = (2, 3, 1, 0)


def neighbours():
    dp, ep = lax.axis_index("dp"), lax.axis_index("ep")
    z_hi, core = dp // 2, dp % 2
    x, z_lo, y = ep // 8, (ep // 4) % 2, ep % 4
    z = z_hi * 2 + z_lo
    a = (1 - core) * x + core * y
    b = (1 - core) * y + core * x

    def device(a, b, z):
        px = (1 - core) * a + core * b
        py = (1 - core) * b + core * a
        return ((z // 2) * 2 + core, (px * 2 + z % 2) * 4 + py)

    up = z + 1 - 2 * (z % 2)
    down = (z + 3 + 2 * (z % 2)) % 4
    zp = (1 - core) * up + core * down
    where = {
        "a+": device((a + 1) % 4, b, z),
        "a-": device((a + 3) % 4, b, z),
        "a2": device((a + 2) % 4, b, z),
        "b2": device(a, (b + 2) % 4, z),
        "b+": device(a, (b + 1) % 4, z),
        "b-": device(a, (b + 3) % 4, z),
        "z": device(a, b, zp),
    }
    return where, ep, where["z"][1]


def kernel(
    tokens, ids_in, nums_in, wg_in, wu_in, wd_in, out,
    wg, wu, wd, T, M, X, ZS, YR, PS, G, H, FAR, ADJ, FFR, FA, SUM, TRI,
    send, recv, local, wsem,
):
    where, ep, pep = neighbours()
    leaving, landing = {}, {}

    def remote(src, dst, to, group, key):
        return pltpu.make_async_remote_copy(
            src_ref=src,
            dst_ref=dst,
            send_sem=send.at[leaving.setdefault(group, len(leaving))],
            recv_sem=recv.at[landing.setdefault(key, len(landing))],
            device_id=where[to],
            device_id_type=MESH,
        )

    def sent(group, ref):
        pltpu.make_async_copy(ref, ref, send.at[leaving[group]]).wait()

    def landed(key, ref):
        pltpu.make_async_copy(ref, ref, recv.at[landing[key]]).wait()

    loads = [
        pltpu.make_async_copy(src, dst, wsem.at[k])
        for k, (src, dst) in enumerate(((wg_in, wg), (wu_in, wu), (wd_in, wd)))
    ]
    own = pltpu.make_async_copy(tokens, T.at[0, 0], local.at[0])
    tables = [
        pltpu.make_async_copy(ids_in, M.at[0, 0, 0, pl.ds(0, 8)], local.at[1]),
        pltpu.make_async_copy(nums_in, M.at[0, 0, 0, pl.ds(8, 8)], local.at[2]),
    ]
    own.start()
    for table in tables:
        table.start()

    mf = [
        remote(M.at[0, 0, 0], M.at[0, 0, 3], "a+", "mf", "mf"),
        remote(M.at[0, 0, 0], M.at[0, 0, 1], "a-", "mf", "mf"),
        remote(M.at[0, 0, 0], M.at[0, 0, 2], "a2", "mf", "mf"),
    ]
    ms = {
        3: remote(M.at[0, 0], M.at[0, 3], "b+", "ms", "ms"),
        1: remote(M.at[0, 0], M.at[0, 1], "b-", "ms", "ms"),
        2: remote(M.at[0, 0], M.at[0, 2], "b2", "ms", "ms"),
    }
    mz = [remote(M.at[0, j], M.at[1, j], "z", "mz", "mz") for j in range(4)]
    f = {}
    for q in range(2):
        part = pl.ds(32 * q, 32)
        f[3, 0, q] = remote(T.at[0, 0, 0, part], T.at[0, 3, 0, part], "a+", "f", ("f", 3, q))
        f[1, 1, q] = remote(T.at[0, 0, 1, part], T.at[0, 1, 1, part], "a+", "f", ("f", 1, q))
        f[2, 0, q] = remote(T.at[0, 3, 0, part], T.at[0, 2, 0, part], "a+", "f", ("f", 2, q))
        f[3, 1, q] = remote(T.at[0, 0, 1, part], T.at[0, 3, 1, part], "a-", "f", ("f", 3, q))
        f[1, 0, q] = remote(T.at[0, 0, 0, part], T.at[0, 1, 0, part], "a-", "f", ("f", 1, q))
        f[2, 1, q] = remote(T.at[0, 3, 1, part], T.at[0, 2, 1, part], "a-", "f", ("f", 2, q))
    s = {}
    for i in range(4):
        s[2, i, 0] = remote(T.at[0, i, 0], T.at[2, i, 0], "b+", "s", ("s", 2, i))
        s[2, i, 1] = remote(T.at[0, i, 1], T.at[2, i, 1], "b-", "s", ("s", 2, i))
        s[1, i, 0] = remote(T.at[2, i, 0], T.at[1, i, 0], "b+", "s", ("s", 1, i))
        s[1, i, 1] = remote(T.at[2, i, 1], T.at[1, i, 1], "b-", "s", ("s", 1, i))
        s[3, i, 1] = remote(T.at[0, i, 1], T.at[3, i, 1], "b+", "s", ("s", 3, i))
        s[3, i, 0] = remote(T.at[0, i, 0], T.at[3, i, 0], "b-", "s", ("s", 3, i))
    zs = {(c, i): remote(ZS.at[c, i], X.at[c, 1, i], "z", "zs", ("zs", c)) for c in range(4) for i in range(4) if c or not i}
    zq = {}
    for i in range(1, 4):
        for q in range(2):
            part = pl.ds(16 * q, 16)
            zq[i, q] = remote(ZS.at[0, i, :, part], X.at[0, 1, i, :, part], "z", "zs", ("zs", 0))
    zr = {(c, i): remote(X.at[c, 1, i], YR.at[c, i], "z", "zr", ("zr", c, i)) for c in range(4) for i in range(4) if (c, i) != (0, 1)}
    zl = []
    for q in range(2):
        part = pl.ds(16 * q, 16)
        zl.append(remote(X.at[0, 1, 1, :, part], YR.at[0, 1, :, part], "z", "zr", ("zl", q)))
    far = {}
    adj = {}
    for i in range(4):
        far[i, 0] = remote(T.at[1, i, 0], FAR.at[i, 0], "b+", "far", ("far", i))
        far[i, 1] = remote(T.at[1, i, 1], FAR.at[i, 1], "b-", "far", ("far", i))
        adj[2, i, 0] = remote(T.at[2, i, 0], ADJ.at[1, i, 0], "b-", "adj", ("adj", i))
        adj[2, i, 1] = remote(T.at[2, i, 1], ADJ.at[0, i, 1], "b+", "adj", ("adj", i))
        adj[3, i, 0] = remote(T.at[3, i, 0], ADJ.at[0, i, 0], "b+", "adj", ("adj", i))
        adj[3, i, 1] = remote(T.at[3, i, 1], ADJ.at[1, i, 1], "b-", "adj", ("adj", i))
    ff = {
        0: remote(T.at[0, 2, 0], FFR.at[0], "a+", "ff", "ff"),
        1: remote(T.at[0, 2, 1], FFR.at[1], "a-", "ff", "ff"),
    }
    fa = {
        (3, 1): remote(T.at[0, 3, 1], FA.at[0, 1], "a+", "fa", "fa"),
        (3, 0): remote(T.at[0, 3, 0], FA.at[1, 0], "a-", "fa", "fa"),
    }
    for q in range(2):
        part = pl.ds(32 * q, 32)
        fa[1, 0, q] = remote(T.at[0, 1, 0, part], FA.at[0, 0, part], "a+", "fa", "fa")
        fa[1, 1, q] = remote(T.at[0, 1, 1, part], FA.at[1, 1, part], "a-", "fa", "fa")

    barrier = pltpu.get_barrier_semaphore()
    peers = ("a+", "a-", "a2", "b+", "b-", "b2", "z")
    for name in peers:
        pl.semaphore_signal(barrier, inc=1, device_id=where[name], device_id_type=MESH)

    lane = lax.broadcasted_iota(jnp.int32, (TOK, TOK), 1)
    row = lax.broadcasted_iota(jnp.int32, (TOK, TOK), 0)
    TRI[...] = jnp.where((row < lane) & ((row & 96) == (lane & 96)), 1.0, 0.0).astype(BF)
    for table in tables:
        table.wait()
    own.wait()
    for load in loads:
        load.start()

    sub8 = lax.broadcasted_iota(jnp.int32, (8, TOK), 0)
    lane8 = lax.broadcasted_iota(jnp.int32, (8, TOK), 1)
    sub32 = lax.broadcasted_iota(jnp.int32, (CAP, TOK), 0).astype(F32)
    expert = jnp.where(sub8 < 2, 2 * ep + sub8, 2 * pep + sub8 - 2)
    start_slot = (((lane8 & 32) >> 1) + ((lane8 & 64) >> 3)).astype(F32)

    low = lax.broadcasted_iota(jnp.int32, (16, TOK), 1) < HALF

    def pick(c, i, plane):
        first, second = ((0, 0), (2, 2), (3, 1), (1, 3))[c]
        return jnp.where(low, M[plane, first, i], M[plane, second, (4 - i) % 4])

    def slots_of(table):
        member = jnp.zeros((8, TOK), F32)
        weight = jnp.zeros((8, TOK), jnp.int32)
        for k in range(8):
            hit = table[k : k + 1] == expert
            member = member + jnp.where(hit, 1.0, 0.0)
            weight = weight + jnp.where(hit, table[8 + k : 9 + k], 0)
        before = jnp.dot(member.astype(BF), TRI[...], preferred_element_type=F32)
        code = jnp.where(member > 0.5, start_slot + before, -1.0)
        return code, weight.astype(F32) * (1.0 / 1024.0)

    def weigh(c, i, plane, hits, gate):
        for e in range(2):
            column = jnp.sum(jnp.where(hits[e], gate[e : e + 1], 0.0), axis=1, keepdims=True)
            G[c, e, plane, i] = jnp.broadcast_to(column, (CAP, TOK))

    def place(c, i):
        code, gate = slots_of(pick(c, i, 0))
        hits = [sub32 == code[r : r + 1] for r in range(4)]
        places = jnp.concatenate([jnp.where(hits[r], 1.0, 0.0) for r in range(4)], axis=0).astype(BF)
        PS[c, i] = places
        weigh(c, i, 0, hits, gate)
        return places

    def pack(c, i):
        places = PS[c, i]
        for n in range(4):
            cols = slice(512 * n, 512 * n + 512)
            rows = T[c, i, :, :, cols].reshape(TOK, 512)
            packed = jnp.dot(places, rows, preferred_element_type=F32).astype(BF)
            X[c, 0, i, :, :, cols] = packed[:HALF].reshape(2, CAP, 512)
            ZS[c, i, :, :, cols] = packed[HALF:].reshape(2, CAP, 512)

    def pack_quarter(i, q):
        part, own = slice(16 * q, 16 * q + 16), slice(32 * q, 32 * q + 32)
        places = jnp.concatenate([PS[0, i, 32 * r + 16 * q : 32 * r + 16 * q + 16] for r in range(4)], axis=0)
        for n in range(4):
            cols = slice(512 * n, 512 * n + 512)
            first, second = T[0, i, 0, own, cols], T[0, i, 1, own, cols]
            rows = jnp.concatenate([first, first, second, second], axis=0)
            packed = jnp.dot(places, rows, preferred_element_type=F32).astype(BF)
            X[0, 0, i, :, part, cols] = packed[:32].reshape(2, 16, 512)
            ZS[0, i, :, part, cols] = packed[32:].reshape(2, 16, 512)
        zq[i, q].start()

    def weigh_theirs(c):
        for i in range(4):
            code, gate = slots_of(pick(c, i, 1))
            weigh(c, i, 1, [sub32 == code[r : r + 1] for r in range(2)], gate)

    def gate_up(c, e, n):
        cols = slice(256 * n, 256 * n + 256) if isinstance(n, int) else pl.ds(pl.multiple_of(n * 256, 256), 256)
        x = X[c, :, :, e].reshape(256, D)
        g = jnp.dot(x, wg[e, :, cols], preferred_element_type=F32)
        u = jnp.dot(x, wu[e, :, cols], preferred_element_type=F32)
        scale = G[c, e].reshape(256, TOK)[:, :1]
        H[:, cols] = (g / (1.0 + jnp.exp(-g)) * u * scale).astype(BF)

    def down(c, e, n):
        cols = pl.ds(pl.multiple_of(n * 512, 512), 512)
        y = jnp.dot(H[...], wd[e, :, cols], preferred_element_type=F32)
        X[c, :, :, e, :, cols] = y.astype(BF).reshape(2, 4, CAP, 512)

    def loop(low, high, step):
        def body(n, carry):
            step(n)
            return carry

        lax.fori_loop(low, high, body, 0)

    def arrived(c):
        landed(("zs", c), X.at[c, 1])
        weigh_theirs(c)

    def fine(c, e):
        return [lambda n=n: gate_up(c, e, n) for n in range(3)] + [
            lambda n=n: loop(n, n + 2, lambda m: down(c, e, m)) for n in (0, 2)
        ]

    def coarse(c, e):
        return [
            lambda: loop(0, 3, lambda n: gate_up(c, e, n)),
            lambda: loop(0, 4, lambda m: down(c, e, m)),
        ]

    def run(steps, count=None):
        for _ in range(len(steps) if count is None else count):
            steps.pop(0)()

    def combine(c, i, extra, target=None):
        for n in range(4):
            cols = slice(512 * n, 512 * n + 512)
            y = jnp.concatenate(
                [X[c, 0, i, :, :, cols].reshape(HALF, 512), YR[c, i, :, :, cols].reshape(HALF, 512)], axis=0
            )
            total = lax.dot_general(PS[c, i], y, (((0,), (0,)), ((), ())), preferred_element_type=F32)
            for part in extra:
                total = total + part[:, :, cols].reshape(TOK, 512).astype(F32)
            if target is None:
                T[c, i, :, :, cols] = total.astype(BF).reshape(2, HALF, 512)
            else:
                target[:, :, cols] = total.reshape(2, HALF, 512)

    def returned(c, i):
        landed(("zr", c, i), YR.at[c, i])
        extra = []
        if c == 3:
            landed(("far", i), FAR.at[i])
            extra = [FAR.at[i]]
        combine(c, i, extra)
        for h in range(2):
            (far[i, h] if c == 1 else adj[c, i, h]).start()

    def pack_send(c, i):
        pack(c, i)
        zs[c, i].start()

    def near(i):
        landed(("s", 2, i), T.at[2, i])
        for h in range(2):
            s[1, i, h].start()
        pack_send(2, i)
        place(1, i)

    def others(i):
        s[3, i, 1].start()
        s[3, i, 0].start()

    def distant(c, i):
        landed(("s", c, i), T.at[c, i])
        pack_send(c, i)
        if c == 1:
            place(3, i)

    place(0, 0)
    pack(0, 0)
    pl.semaphore_wait(barrier, len(peers))
    for q in range(2):
        f[3, 0, q].start()
        f[3, 1, q].start()
        if q == 0:
            for copy in mf:
                copy.start()
            zs[0, 0].start()
    for q in range(2):
        f[1, 1, q].start()
        f[1, 0, q].start()
    for q in range(2):
        landed(("f", 3, q), T.at[0, 3, :, pl.ds(32 * q, 32)])
        for h in range(2):
            f[2, h, q].start()
        if q == 0:
            landed("mf", M.at[0, 0, pl.ds(1, 3)])
            place(0, 3)
            for j in (1, 3, 2):
                ms[j].start()
        pack_quarter(3, q)
    place(0, 1)
    for q in range(2):
        landed(("f", 1, q), T.at[0, 1, :, pl.ds(32 * q, 32)])
        for i in ((), (0, 3, 1))[q]:
            s[2, i, 0].start()
            s[2, i, 1].start()
        pack_quarter(1, q)
    mz[0].start()
    landed("ms", M.at[0, pl.ds(1, 3)])
    for j in (1, 3, 2):
        mz[j].start()
    place(0, 2)
    for i in ORDER:
        place(2, i)
    for q in range(2):
        landed(("f", 2, q), T.at[0, 2, :, pl.ds(32 * q, 32)])
        pack_quarter(2, q)
    s[2, 2, 0].start()
    s[2, 2, 1].start()
    near(0)
    near(3)
    others(0)
    near(1)
    others(3)
    near(2)
    others(1)
    others(2)
    distant(1, 0)
    landed("mz", M.at[1])
    for load in loads:
        load.wait()
    arrived(0)
    first = fine(0, 0)
    run(first, 2)
    distant(1, 3)
    run(first, 2)
    distant(3, 0)
    run(first)
    distant(1, 1)
    arrived(2)
    second = fine(2, 0) + fine(2, 1)
    run(second, 2)
    distant(3, 3)
    run(second, 3)
    distant(1, 2)
    run(second, 2)
    distant(3, 1)
    run(second)
    distant(3, 2)
    for i in BACK:
        zr[2, i].start()
    sent("f", T.at[0, pl.ds(0, 3)])
    sent("s", T.at[pl.ds(0, 3)])
    arrived(1)
    run(coarse(1, 0) + coarse(1, 1))
    arrived(3)
    for i in BACK:
        zr[1, i].start()
    returned(2, 2)
    third = coarse(3, 0) + coarse(3, 1)
    run(third, 1)
    returned(2, 3)
    run(third, 1)
    returned(2, 1)
    run(third, 1)
    returned(2, 0)
    run(third)
    zr[3, 2].start()
    zr[3, 3].start()
    returned(1, 2)
    last = coarse(0, 1)
    run(last, 1)
    returned(1, 3)
    run(last)
    returned(1, 1)
    returned(1, 0)
    zr[3, 1].start()
    zr[0, 2].start()

    def finish(i, extra, target=None):
        landed(("zr", 0, i), YR.at[0, i])
        landed(("adj", i), ADJ.at[:, i])
        combine(0, i, [ADJ.at[0, i], ADJ.at[1, i]] + extra, target)

    returned(3, 2)
    zr[3, 0].start()
    returned(3, 3)
    zr[0, 3].start()
    returned(3, 1)
    zl[0].start()
    zl[1].start()
    finish(2, [])
    ff[0].start()
    ff[1].start()
    zr[0, 0].start()
    returned(3, 0)
    finish(3, [])
    fa[3, 0].start()
    fa[3, 1].start()
    landed(("adj", 1), ADJ.at[:, 1])
    landed("ff", FFR)
    for n in range(4):
        cols = slice(512 * n, 512 * n + 512)
        known = [ref[:, :, cols].astype(F32) for ref in (ADJ.at[0, 1], ADJ.at[1, 1], FFR)]
        SUM[:, :, cols] = known[0] + known[1] + known[2]
    for q in range(2):
        landed(("zl", q), YR.at[0, 1, :, pl.ds(16 * q, 16)])
        part, own = slice(16 * q, 16 * q + 16), slice(32 * q, 32 * q + 32)
        places = jnp.concatenate([PS[0, 1, 32 * r + 16 * q : 32 * r + 16 * q + 16] for r in range(4)], axis=0)
        for n in range(4):
            cols = slice(512 * n, 512 * n + 512)
            y = jnp.concatenate(
                [X[0, 0, 1, :, part, cols].reshape(32, 512), YR[0, 1, :, part, cols].reshape(32, 512)], axis=0
            )
            total = lax.dot_general(places, y, (((0,), (0,)), ((), ())), preferred_element_type=F32)
            for h in range(2):
                rows = total[64 * h + 32 * q : 64 * h + 32 * q + 32]
                T[0, 1, h, own, cols] = (rows + SUM[h, own, cols]).astype(BF)
        fa[1, 0, q].start()
        fa[1, 1, q].start()
    finish(0, [], SUM)
    landed("fa", FA)
    for n in range(4):
        cols = slice(512 * n, 512 * n + 512)
        total = SUM[:, :, cols] + FA[0, :, :, cols].astype(F32) + FA[1, :, :, cols].astype(F32)
        out[:, cols] = total.astype(BF).reshape(TOK, 512)

    for group, ref in (
        ("mf", M.at[0, 0, pl.ds(0, 3)]), ("ms", M.at[0, pl.ds(0, 3)]), ("mz", M.at[0]), ("zs", ZS), ("zr", YR),
        ("far", FAR), ("adj", ADJ), ("ff", FFR), ("fa", FA),
    ):
        sent(group, ref)


GROUPS = 11
KEYS = 3 + 6 + 12 + 4 + 17 + 4 + 4 + 2


def shards(tokens, expert_ids, gate_nums, w_gate, w_up, w_down):
    anywhere = pl.BlockSpec(memory_space=pl.ANY)
    return pl.pallas_call(
        kernel,
        name="routed_experts",
        out_shape=pltpu.VMEM((TOK, D), BF),
        in_specs=[anywhere] * 6,
        out_specs=pl.BlockSpec(memory_space=pltpu.VMEM),
        scratch_shapes=[
            pltpu.VMEM((2, D, FF), BF),
            pltpu.VMEM((2, D, FF), BF),
            pltpu.VMEM((2, FF, D), BF),
            pltpu.VMEM((4, 4, 2, HALF, D), BF),
            pltpu.VMEM((2, 4, 4, 16, TOK), jnp.int32),
            pltpu.VMEM((4, 2, 4, 2, CAP, D), BF),
            pltpu.VMEM((4, 4, 2, CAP, D), BF),
            pltpu.VMEM((4, 4, 2, CAP, D), BF),
            pltpu.VMEM((4, 4, TOK, TOK), BF),
            pltpu.VMEM((4, 2, 2, 4, CAP, TOK), F32),
            pltpu.VMEM((256, FF), BF),
            pltpu.VMEM((4, 2, HALF, D), BF),
            pltpu.VMEM((2, 4, 2, HALF, D), BF),
            pltpu.VMEM((2, HALF, D), BF),
            pltpu.VMEM((2, 2, HALF, D), BF),
            pltpu.VMEM((2, HALF, D), F32),
            pltpu.VMEM((TOK, TOK), BF),
            pltpu.SemaphoreType.DMA((GROUPS,)),
            pltpu.SemaphoreType.DMA((KEYS,)),
            pltpu.SemaphoreType.DMA((3,)),
            pltpu.SemaphoreType.DMA((3,)),
        ],
        compiler_params=pltpu.CompilerParams(
            collective_id=0, has_side_effects=True, vmem_limit_bytes=62 * 1024 * 1024
        ),
    )(tokens.reshape(2, HALF, D), expert_ids.T, gate_nums.T, w_gate, w_up, w_down)


def solution(mesh):
    placed = (
        P(("dp", "ep"), None),
        P(("dp", "ep"), None),
        P(("dp", "ep"), None),
        P("ep", None, None),
        P("ep", None, None),
        P("ep", None, None),
    )
    return jax.shard_map(
        shards, mesh=mesh, in_specs=placed, out_specs=P(("dp", "ep"), None), check_vma=False
    )
```
